32 devices in a mesh: rep: 1, r: 8 (over y, z), s: 4 (over x, core).
Axes of the slice: x: 2, y: 2, z: 4, core: 2. Of those that a mesh axis runs over, the one named last changes fastest.
Arguments:
- x: bfloat16 [32, 4096, 512], P(('rep', 'r', 's'))
- dy: bfloat16 [32, 4096, 512], P(('rep', 'r', 's'))
- w_gate: bfloat16 [2, 512, 1280], P(None, 's')
- w_up: bfloat16 [2, 512, 1280], P(None, 's')
- w_down: bfloat16 [2, 1280, 512], P(None, 's')
- m_w_gate: float32 [2, 512, 1280], P(None, 's')
- m_w_up: float32 [2, 512, 1280], P(None, 's')
- m_w_down: float32 [2, 1280, 512], P(None, 's')
- v_w_gate: float32 [2, 512, 1280], P(None, 's')
- v_w_up: float32 [2, 512, 1280], P(None, 's')
- v_w_down: float32 [2, 1280, 512], P(None, 's')
Outputs:
- output 1: bfloat16 [2, 512, 1280], P('rep', 's')
- output 2: bfloat16 [2, 512, 1280], P('rep', 's')
- output 3: bfloat16 [2, 1280, 512], P('rep', 's')
- output 4: float32 [2, 512, 1280], P('rep', 's')
- output 5: float32 [2, 512, 1280], P('rep', 's')
- output 6: float32 [2, 1280, 512], P('rep', 's')
- output 7: float32 [2, 512, 1280], P('rep', 's')
- output 8: float32 [2, 512, 1280], P('rep', 's')
- output 9: float32 [2, 1280, 512], P('rep', 's')
All inputs are finite; a program needn't handle non-finite values.
Results may differ from the reference program's by a relative error of at most 0.022.
Values are sent between devices in bfloat16 or wider.
A program may use at most 2 GiB of HBM per device.

```python
import jax
import jax.numpy as jnp
from jax import lax

SEQUENCES = 32
TOKENS = 4096
D = 512
FF = 1280
LAYERS = 2
NAMES = ("w_gate", "w_up", "w_down")
SHAPES = {"w_gate": (LAYERS, D, FF), "w_up": (LAYERS, D, FF), "w_down": (LAYERS, FF, D)}


def bump(key, n, height):
    away = (jnp.arange(n, dtype=jnp.int32) - jax.random.randint(key, (), 0, n, jnp.int32)) % n
    return jnp.where(away < n // 8, height, 1.0)


def together(key, own, strength):
    shared = jax.random.normal(key, own.shape[1:], jnp.float32)
    return (own + strength * shared) * lax.rsqrt(1 + strength * strength)


def setup_inputs(seed: int = 0, part: int = 0) -> dict:
    kx, kdy, ka, kb, kz, kf, kh, kl, *keys = jax.random.split(jax.random.key(seed), 8 + 3 * len(NAMES))
    kx, kdy, ka, kb = (jax.random.fold_in(k, part) for k in (kx, kdy, ka, kb))
    kw, km, kv = (keys[i::3] for i in range(3))
    shape = (SEQUENCES, TOKENS, D)
    much_x, much_dy = jax.random.uniform(kz, (2,), jnp.float32, 0.0, 1.0)
    loud = 2.0 ** jax.random.uniform(jax.random.fold_in(kz, 1), (), jnp.float32, -1.0, 2.0)
    layers = 2.0 ** jax.random.uniform(kl, (LAYERS, 1, 1), jnp.float32, -1.0, 1.0)
    x = together(ka, jax.random.normal(kx, shape, jnp.float32), much_x) * bump(kf, D, 4.0)
    dy = together(kb, jax.random.normal(kdy, shape, jnp.float32), much_dy)
    drawn = {"x": x.astype(jnp.bfloat16), "dy": (loud * dy * (SEQUENCES * TOKENS) ** -0.5).astype(jnp.bfloat16)}
    for key, name in zip(kw, NAMES, strict=True):
        w = jax.random.normal(key, SHAPES[name], jnp.float32) * SHAPES[name][1] ** -0.5
        drawn[name] = (w * {"w_gate": 1.0, "w_up": bump(kh, FF, 4.0), "w_down": layers}[name]).astype(jnp.bfloat16)
    for key, name in zip(km, NAMES, strict=True):
        drawn[f"m_{name}"] = 0.1 * jax.random.normal(key, SHAPES[name], jnp.float32)
    for key, name in zip(kv, NAMES, strict=True):
        drawn[f"v_{name}"] = jax.random.uniform(key, SHAPES[name], jnp.float32, 0.005, 0.015)
    return drawn


def matmul(a, w):
    return jnp.dot(a, w, preferred_element_type=jnp.float32).astype(jnp.bfloat16)


def normed(h):
    wide = h.astype(jnp.float32)
    scale = lax.rsqrt(jnp.mean(wide**2, -1, keepdims=True) + 1e-6)
    return (wide * scale).astype(jnp.bfloat16)


def layer(h, w):
    a = normed(h)
    gate = jnp.dot(a, w["w_gate"], preferred_element_type=jnp.float32)
    up = jnp.dot(a, w["w_up"], preferred_element_type=jnp.float32)
    return h + matmul((jax.nn.silu(gate) * up).astype(jnp.bfloat16), w["w_down"])


def adamw(w, m, v, g):
    m = 0.9 * m + 0.1 * g
    v = 0.95 * v + 0.05 * g * g
    step = m * lax.rsqrt(v + 1e-8) + 0.1 * w
    return (w - 0.02 * step).astype(jnp.bfloat16), m, v


def clipped(gradients, sum_of_squares, count):
    factor = jnp.minimum(1.0, 0.5 * lax.rsqrt(sum_of_squares / count + 1e-30))
    return [g * factor for g in gradients]


def stack(weights, h):
    return lax.scan(lambda h, w: (layer(h, w), None), h, weights)[0]


def reference(x, dy, w_gate, w_up, w_down, m_w_gate, m_w_up, m_w_down, v_w_gate, v_w_up, v_w_down):
    weights = dict(zip(NAMES, (w_gate, w_up, w_down), strict=True))

    def take(so_far, sequence):
        h, by_y = sequence
        _, back = jax.vjp(lambda w: stack(w, h), weights)
        return jax.tree.map(lambda total, term: total + term.astype(jnp.float32), so_far, back(by_y)[0]), None

    none_yet = {name: jnp.zeros(w.shape, jnp.float32) for name, w in weights.items()}
    by_weights, _ = lax.scan(take, none_yet, (x, dy))
    gradients = [by_weights[name].astype(jnp.bfloat16).astype(jnp.float32) for name in NAMES]
    gradients = clipped(gradients, sum(jnp.sum(g * g) for g in gradients), sum(g.size for g in gradients))
    new = [
        adamw(w.astype(jnp.float32), m, v, g)
        for w, m, v, g in zip((w_gate, w_up, w_down), (m_w_gate, m_w_up, m_w_down), (v_w_gate, v_w_up, v_w_down), gradients, strict=True)
    ]
    return tuple(one[which] for which in range(3) for one in new)
```

```python
import functools

import jax
import jax.numpy as jnp
from jax import lax
from jax.experimental import pallas as pl
from jax.experimental.pallas import tpu as pltpu
from jax.sharding import PartitionSpec as P

MESH = pl.DeviceIdType.MESH
BF, F32 = jnp.bfloat16, jnp.float32
T, D, FF, L = 4096, 512, 1280, 2
TB, FC = 512, 256
NT, NC = T // TB, FF // FC
TBB = 1024
BB = T // TBB
G = L * NC
DS, FS = D // 4, FF // 4


def dot(a, b):
    return jnp.dot(a, b, preferred_element_type=F32)


def dot_t(a, b):
    return lax.dot_general(a, b, (((1,), (1,)), ((), ())), preferred_element_type=F32)


def sigmoid(g):
    return 0.5 + 0.5 * jnp.tanh(0.5 * g)


def norm_scale(wide):
    return lax.rsqrt(jnp.mean(wide * wide, -1, keepdims=True) + 1e-6)


def aligned(i, n):
    return pl.multiple_of(i * n, n)


def kernel(x_in, dy_in, wg_in, wu_in, wd_in, gu_out, d_out, sq_out, *scratch):
    (hb, dyb, a0, a1, a0t, a1t, dyt, da, wgu, wd, acc, sbg, sbd, r0g, r0d, t1g, t1d, r1g, r1d, o32g, o32d, s2g, s2d, r2g, r2d,
     fg, fd, gfin, dfin, sq, ld, wla, wcs, wcr, wxs, wxr, wys, wyr, was, war, wbs, wbr,
     s0s, s0r, s1s, s1r, s2s, s2r, s3s, s3r, s3ds, s3dr, sqs, sqr, osem) = scratch
    s, r = lax.axis_index("s"), lax.axis_index("r")
    xx, cc, yy = s // 2, s % 2, r // 4
    s1, s2, s3 = 2 * xx + 1 - cc, 2 * (1 - xx) + cc, 2 * (1 - xx) + 1 - cc
    across = (r + 4) % 8

    def remote(src, dst, send, recv, rr, ss):
        return pltpu.make_async_remote_copy(
            src_ref=src, dst_ref=dst, send_sem=send, recv_sem=recv, device_id={"r": rr, "s": ss}, device_id_type=MESH
        )

    barrier = pltpu.get_barrier_semaphore()
    for dr in (0, 4, 1, 7, 5, 3, 2, 6):
        for ds in range(4):
            if (dr, ds) != (0, 0):
                pl.semaphore_signal(barrier, inc=1, device_id={"r": (r + dr) % 8, "s": (s + ds) % 4}, device_id_type=MESH)

    WIDE = (512, 768)

    def first(part, x):
        return pl.multiple_of((1 - x) * 512, 256) if part else pl.multiple_of(x * 768, 256)

    def shard_in(j):
        return (wg_in, wu_in, wd_in)[j % 3].at[j // 3]

    def region(j, who):
        if j % 3 < 2:
            return wgu.at[j // 3, j % 3, pl.ds(aligned(who, DS), DS), :]
        return wd.at[j // 3, pl.ds(aligned(who, FS), FS), :]

    def own(j):
        return pltpu.make_async_copy(shard_in(j), region(j, s), wla.at[j])

    def to_core(j):
        return remote(region(j, s), region(j, s), wcs.at[j], wcr.at[j], r, s1)

    def half_of(j, who, half, x):
        if j < 4:
            return wgu.at[0, j % 2, pl.ds(aligned(2 * who + half, 64), 64), pl.ds(first(j // 2, x), WIDE[j // 2])]
        if j in (5, 6):
            return wgu.at[1, j - 5, pl.ds(aligned(2 * who + half, 64), 64), :]
        return wd.at[(j - 4) // 3, pl.ds(aligned(2 * who + half, 160), 160), :]

    def by_x(j):
        return remote(half_of(j, s, yy, 1 - xx), half_of(j, s, yy, 1 - xx), wxs.at[j], wxr.at[j], r, s2)

    def by_y(j):
        return remote(half_of(j, s2, yy, xx), half_of(j, s2, yy, xx), wys.at[j], wyr.at[j], across, s)

    def by_core(j, half, send, recv):
        return remote(half_of(j, s2, half, xx), half_of(j, s2, half, xx), send.at[j], recv.at[j], r, s1)

    def got_x(j):
        by_x(j).wait_recv()
        by_y(j).start()
        by_core(j, yy, was, war).start()

    def got_y(j):
        by_y(j).wait_recv()
        by_core(j, 1 - yy, wbs, wbr).start()

    def got_core(j):
        by_core(j, yy, was, war).wait_recv()
        by_core(j, 1 - yy, wbs, wbr).wait_recv()

    for j in range(6):
        own(j).start()
    load_x = pltpu.make_async_copy(x_in.at[0], hb, ld.at[0])
    load_dy = pltpu.make_async_copy(dy_in.at[0], dyb, ld.at[1])
    load_x.start()
    load_dy.start()
    for j in range(6):
        own(j).wait()
    pl.semaphore_wait(barrier, 31)
    for j in range(8):
        by_x(j).start()
    for j in range(6):
        to_core(j).start()
    load_x.wait()
    load_dy.wait()

    def prologue(i, _):
        rows = pl.ds(aligned(i, TB), TB)
        wide = hb[rows, :].astype(F32)
        a = (wide * norm_scale(wide)).astype(BF)
        a0[rows, :] = a
        a0t[:, rows] = a.T
        dyt[:, rows] = dyb[rows, :].T

        @pl.when(i == 4)
        def _():
            got_x(0)
            got_x(1)

        return 0

    lax.fori_loop(0, NT, prologue, 0)

    def mlp(a, start, width):
        o = None
        for c in range(width // FC):
            cols = pl.ds(pl.multiple_of(start + c * FC, FC), FC)
            g = dot(a, wgu[0, 0, :, cols])
            u = dot(a, wgu[0, 1, :, cols])
            p = (g * sigmoid(g) * u).astype(BF)
            one = dot(p, wd[0, cols, :])
            o = one if o is None else o + one
        return o

    def fwd_first(i, _):
        @pl.when(i == 2)
        def _():
            got_x(3)
            got_y(2)

        @pl.when(i == 5)
        def _():
            got_x(4)
            got_y(3)

        rows = pl.ds(aligned(i, TB), TB)
        da[rows, :] = mlp(a0[rows, :], first(0, xx), WIDE[0])
        return 0

    def fwd_second(i, _):
        @pl.when(i == 4)
        def _():
            for j in (5, 6, 7):
                got_x(j)

        @pl.when(i == 7)
        def _():
            for j in (5, 6, 7):
                got_y(j)

        rows = pl.ds(aligned(i, TB), TB)
        o = da[rows, :] + mlp(a0[rows, :], first(1, xx), WIDE[1])
        da[rows, :] = jnp.zeros((TB, D), F32)
        h = hb[rows, :] + o.astype(BF)
        hb[rows, :] = h
        wide = h.astype(F32)
        a = (wide * norm_scale(wide)).astype(BF)
        a1[rows, :] = a
        a1t[:, rows] = a.T
        return 0

    got_y(0)
    got_y(1)
    got_x(2)
    for j in range(3):
        to_core(j).wait_recv()
    got_core(0)
    got_core(1)
    lax.fori_loop(0, NT, fwd_first, 0)
    got_y(4)
    for j in (2, 3, 4):
        got_core(j)
    lax.fori_loop(0, NT, fwd_second, 0)
    for j in range(3, 6):
        to_core(j).wait_recv()
    for j in (5, 6, 7):
        got_core(j)

    def part(m, who):
        return pl.ds(aligned(who, 64), 64) if m == 2 else pl.ds(aligned(who, DS), DS)

    def mine(m, gu, d):
        return (lambda g, *at: d.at[(g, *at)]) if m == 2 else (lambda g, *at: gu.at[(g, m, *at)])

    def stage0(g, m, w):
        slot = g % 2
        src = mine(m, sbg, sbd)(slot, part(m, (s1, s3)[w]), slice(None))
        return remote(src, mine(m, r0g, r0d)(slot, w), s0s.at[slot, m // 2], s0r.at[slot, 2 * m + w], r, s1)

    def stage0_sent(g):
        slot = g % 2
        pltpu.make_async_copy(r0g.at[slot], r0g.at[slot], s0s.at[slot, 0]).wait()
        pltpu.make_async_copy(r0d.at[slot], r0d.at[slot], s0s.at[slot, 1]).wait()

    def stage1(g, m):
        return remote(mine(m, t1g, t1d)(g % 2), mine(m, r1g, r1d)(g), s1s.at[g % 2, m], s1r.at[g, m], r, s2)

    def piece(m, who):
        if m == 2:
            return pl.ds(aligned(who // 2, 16), 16), pl.ds(aligned(who % 2, 256), 256)
        return pl.ds(aligned(who, 16), 16), slice(None)

    def stage2(g, m, k):
        to = (r + k) % 8
        return remote(
            mine(m, s2g, s2d)(g, *piece(m, to)), mine(m, r2g, r2d)(g, k - 1), s2s.at[m // 2], s2r.at[g, 7 * m + k - 1], to, s
        )

    def place(g):
        block = 4 * (g % NC) + s
        spot = pl.ds(aligned(4 * (block % 5) + r // 2, 16), 16), pl.ds(aligned(r % 2, 256), 256)
        return 1 - g // NC, g % NC, block // 5, spot

    def stage3(g, m, k):
        to = (r + k) % 8
        layer, c, owner, spot = place(g)
        if m == 2:
            return remote(fd.at[g], dfin.at[(layer, *spot)], s3ds, s3dr, to, owner)
        return remote(fg.at[g, m], gfin.at[layer, m, pl.ds(aligned(r, 16), 16), pl.ds(aligned(c, FC), FC)], s3s, s3r, to, s)

    def add0(g, m, fresh):
        slot = g % 2
        for w in (1, 0):
            stage0(g, m, w).wait_recv()
        if not fresh:
            stage1(g, m).wait_send()
        own_term = mine(m, sbg, sbd)
        arrived = mine(m, r0g, r0d)
        other = own_term(slot, part(m, s2), slice(None))[...].astype(F32) + arrived(slot, 1)[...].astype(F32)
        mine(m, t1g, t1d)(slot)[...] = other.astype(BF)
        stage1(g, m).start()
        kept = own_term(slot, part(m, s), slice(None))[...].astype(F32) + arrived(slot, 0)[...].astype(F32)
        mine(m, o32g, o32d)(g % 4)[...] = kept

    def add1(g, m):
        stage1(g, m).wait_recv()
        total = mine(m, o32g, o32d)(g % 4)[...] + mine(m, r1g, r1d)(g)[...].astype(F32)
        mine(m, o32g, o32d)(g % 4)[...] = total
        mine(m, s2g, s2d)(g)[...] = total.astype(BF)
        for k in (4, 5, 3, 6, 2, 7, 1):
            stage2(g, m, k).start()

    def add2(g, m):
        for k in range(1, 8):
            stage2(g, m, k).wait_recv()
        total = mine(m, o32g, o32d)(g % 4, *piece(m, r))[...]
        for k in range(7):
            total += mine(m, r2g, r2d)(g, k)[...].astype(F32)
        total = total.astype(BF)
        mine(m, fg, fd)(g)[...] = total
        layer, c, owner, spot = place(g)
        if m == 2:

            @pl.when(owner == s)
            def _():
                dfin[(layer, *spot)] = total

            @pl.when(owner != s)
            def _():
                stage3(g, m, 0).start()
        else:
            gfin[layer, m, pl.ds(aligned(r, 16), 16), pl.ds(aligned(c, FC), FC)] = total
        for k in (4, 5, 3, 6, 2, 7, 1):
            stage3(g, m, k).start()

    def backward(layer, a_ref, at_ref, with_da):
        def chunk(c, _):
            cols = pl.ds(aligned(c, FC), FC)
            n = (1 - layer) * NC + c

            def block(i, _):
                @pl.when((i == 1) & (n >= 3))
                def _():
                    for m in range(3):
                        add0(n - 1, m, False)

                @pl.when((i == 1) & (n >= 1) & (n < 3))
                def _():
                    for m in range(3):
                        add0(n - 1, m, True)

                @pl.when((i == BB - 1) & (n >= 2))
                def _():
                    for m in range(3):
                        add2(n - 2, m)

                @pl.when((i == BB - 1) & (n >= 1))
                def _():
                    for m in range(3):
                        add1(n - 1, m)

                rows = pl.ds(aligned(i, TBB), TBB)
                a = a_ref[rows, :]
                g = dot(a, wgu[layer, 0, :, cols])
                u = dot(a, wgu[layer, 1, :, cols])
                dp = dot_t(dyb[rows, :], wd[layer, cols, :]).astype(BF).astype(F32)
                sig = sigmoid(g)
                sl = g * sig
                p = (sl * u).astype(BF)
                du = (dp * sl).astype(BF)
                dg = (dp * u * (sig + sl * (1.0 - sig))).astype(BF)
                for m, (left, right) in enumerate(((at_ref, dg), (at_ref, du), (dyt, p))):
                    acc[m] = jnp.where(i > 0, acc[m], 0.0) + dot(left[:, rows], right)
                if with_da:
                    da[rows, :] += dot_t(dg, wgu[layer, 0, :, cols]) + dot_t(du, wgu[layer, 1, :, cols])
                return 0

            lax.fori_loop(0, BB, block, 0)
            slot = n % 2

            @pl.when(n >= 2)
            def _():
                stage0_sent(n)

            for m in range(3):
                mine(m, sbg, sbd)(slot)[...] = (acc[m].T if m == 2 else acc[m]).astype(BF)
                for w in (1, 0):
                    stage0(n, m, w).start()
            return 0

        lax.fori_loop(0, NC, chunk, 0)

    backward(1, a1, a1t, True)

    def norm_back(i, _):
        rows = pl.ds(aligned(i, TB), TB)
        wide = hb[rows, :].astype(F32)
        scale = norm_scale(wide)
        t = da[rows, :].astype(BF).astype(F32)
        back = scale * t - wide * (scale * scale * scale * jnp.mean(t * wide, -1, keepdims=True))
        dh = dyb[rows, :] + back.astype(BF)
        dyb[rows, :] = dh
        dyt[:, rows] = dh.T
        return 0

    lax.fori_loop(0, NT, norm_back, 0)
    backward(0, a0, a0t, False)

    for m in range(3):
        add0(G - 1, m, False)
    for m in range(3):
        add2(G - 2, m)
    for m in range(3):
        add1(G - 1, m)
    for m in range(3):
        add2(G - 1, m)

    def bytes_of(ref, sem):
        pltpu.make_async_copy(ref, ref, sem).wait()

    bytes_of(gfin.at[:, :, 0 : 7 * 16, :], s3r)
    bytes_of(dfin.at[:, 0:304, :], s3dr)
    out_g = pltpu.make_async_copy(gfin, gu_out, osem.at[0])
    out_d = pltpu.make_async_copy(dfin, d_out, osem.at[1])
    out_g.start()
    out_d.start()

    def squares(n, width, read):
        def one(i, total):
            v = read(i).astype(F32)
            return total + jnp.sum((v * v).reshape(n // 8, 8, width), axis=0)

        return one

    tg = jnp.zeros((8, FF), F32)
    td = jnp.zeros((8, D), F32)
    for layer in range(L):
        for m in range(2):
            tg = lax.fori_loop(0, DS // 32, squares(32, FF, lambda i: gfin[layer, m, pl.ds(aligned(i, 32), 32), :]), tg)
        td = lax.fori_loop(0, FS // 64, squares(64, D, lambda i: dfin[layer, pl.ds(aligned(i, 64), 64), :]), td)
    total = jnp.zeros((8, 128), F32)
    for j in range(FF // 128):
        total += tg[:, 128 * j : 128 * j + 128]
    for j in range(D // 128):
        total += td[:, 128 * j : 128 * j + 128]
    sq[s] = total

    def share(k, whose):
        return remote(sq.at[s], sq.at[whose], sqs.at[k - 1], sqr.at[k - 1], r, (s + k) % 4)

    for k in (2, 3, 1):
        share(k, s).start()
    for j in range(6):
        to_core(j).wait_send()
    for j in range(8):
        by_x(j).wait_send()
        by_y(j).wait_send()
        by_core(j, yy, was, war).wait_send()
        by_core(j, 1 - yy, wbs, wbr).wait_send()
    stage0_sent(G - 2)
    stage0_sent(G - 1)
    for m in range(3):
        stage1(G - 2, m).wait_send()
        stage1(G - 1, m).wait_send()
    bytes_of(r2g, s2s.at[0])
    bytes_of(r2d, s2s.at[1])
    bytes_of(gfin.at[:, :, 0 : 7 * 16, :], s3s)
    bytes_of(dfin.at[:, 0:304, :], s3ds)
    for k in (1, 2, 3):
        share(k, (s + 4 - k) % 4).wait()
    sq_out[...] = ((sq[0] + sq[1]) + sq[2]) + sq[3]
    out_g.wait()
    out_d.wait()


def adamw(w, m, v, g):
    m = 0.9 * m + 0.1 * g
    v = 0.95 * v + 0.05 * g * g
    step = m * lax.rsqrt(v + 1e-8) + 0.1 * w
    return (w - 0.02 * step).astype(BF), m, v


def solution(mesh):
    def step(x, dy, *arrays):
        weights, ms, vs = (arrays[i : i + 3] for i in (0, 3, 6))
        hbm = pl.BlockSpec(memory_space=pl.ANY)
        dma = pltpu.SemaphoreType.DMA
        gu, d, sq = pl.pallas_call(
            kernel,
            name="train_step",
            out_shape=(
                jax.ShapeDtypeStruct((L, 2, DS, FF), BF),
                jax.ShapeDtypeStruct((L, FS, D), BF),
                jax.ShapeDtypeStruct((8, 128), F32),
            ),
            in_specs=[hbm] * 5,
            out_specs=(hbm, hbm, pl.BlockSpec(memory_space=pltpu.VMEM)),
            scratch_shapes=[
                pltpu.VMEM((T, D), BF),
                pltpu.VMEM((T, D), BF),
                pltpu.VMEM((T, D), BF),
                pltpu.VMEM((T, D), BF),
                pltpu.VMEM((D, T), BF),
                pltpu.VMEM((D, T), BF),
                pltpu.VMEM((D, T), BF),
                pltpu.VMEM((T, D), F32),
                pltpu.VMEM((L, 2, D, FF), BF),
                pltpu.VMEM((L, FF, D), BF),
                pltpu.VMEM((3, D, FC), F32),
                pltpu.VMEM((2, 2, D, FC), BF),
                pltpu.VMEM((2, FC, D), BF),
                pltpu.VMEM((2, 2, 2, DS, FC), BF),
                pltpu.VMEM((2, 2, FC // 4, D), BF),
                pltpu.VMEM((2, 2, DS, FC), BF),
                pltpu.VMEM((2, FC // 4, D), BF),
                pltpu.VMEM((G, 2, DS, FC), BF),
                pltpu.VMEM((G, FC // 4, D), BF),
                pltpu.VMEM((4, 2, DS, FC), F32),
                pltpu.VMEM((4, FC // 4, D), F32),
                pltpu.VMEM((G, 2, DS, FC), BF),
                pltpu.VMEM((G, FC // 4, D), BF),
                pltpu.VMEM((G, 2, 7, 16, FC), BF),
                pltpu.VMEM((G, 7, 16, 256), BF),
                pltpu.VMEM((G, 2, 16, FC), BF),
                pltpu.VMEM((G, 16, 256), BF),
                pltpu.VMEM((L, 2, DS, FF), BF),
                pltpu.VMEM((L, FS, D), BF),
                pltpu.VMEM((4, 8, 128), F32),
                dma((2,)),
                dma((6,)), dma((6,)), dma((6,)),
                dma((8,)), dma((8,)), dma((8,)), dma((8,)), dma((8,)), dma((8,)), dma((8,)), dma((8,)),
                dma((2, 2)), dma((2, 6)), dma((2, 3)), dma((G, 3)),
                dma((2,)), dma((G, 21)),
                dma(()), dma(()), dma(()), dma(()),
                dma((3,)), dma((3,)), dma((2,)),
            ],
            compiler_params=pltpu.CompilerParams(collective_id=0, has_side_effects=True, vmem_limit_bytes=67043328),
        )(x, dy, *weights)
        count = 4 * (gu.size + d.size)
        factor = jnp.minimum(1.0, 0.5 * lax.rsqrt(jnp.sum(sq) / count + 1e-30))
        grads = (gu[:, 0], gu[:, 1], d)
        new = [adamw(w.astype(F32), m, v, g.astype(F32) * factor) for w, m, v, g in zip(weights, ms, vs, grads, strict=True)]
        return tuple(one[which] for which in range(3) for one in new)

    states, cut = P(("rep", "r", "s"), None, None), P(None, "s", None)
    return jax.shard_map(
        step, mesh=mesh, in_specs=(states, states) + (cut,) * 9, out_specs=(P("rep", "s", None),) * 9, check_vma=False
    )
```

```python
import functools

import jax
import jax.numpy as jnp
from jax import lax
from jax.experimental import pallas as pl
from jax.experimental.pallas import tpu as pltpu
from jax.sharding import PartitionSpec as P

MESH = pl.DeviceIdType.MESH
BF, F32 = jnp.bfloat16, jnp.float32
T, D, FF, L = 4096, 512, 1280, 2
TB, FC = 512, 256
NT, NC = T // TB, FF // FC
TBB, SB = 1024, 256
BB = T // TBB
G = L * NC
STEPS = 4
DS, FS = D // 4, FF // 4


def dot(a, b):
    return jnp.dot(a, b, preferred_element_type=F32)


def dot_t(a, b):
    return lax.dot_general(a, b, (((1,), (1,)), ((), ())), preferred_element_type=F32)


def sigmoid(g):
    return 0.5 + 0.5 * jnp.tanh(0.5 * g)


def norm_scale(wide):
    return lax.rsqrt(jnp.mean(wide * wide, -1, keepdims=True) + 1e-6)


def aligned(i, n):
    return pl.multiple_of(i * n, n)


def kernel(x_in, dy_in, wg_in, wu_in, wd_in, gu_out, d_out, sq_out, *scratch):
    (hb, dyb, a0, a1, a0t, a1t, dyt, da, wgu, wd, acc, sbg, sbd, r0g, r0d, t1g, t1d, r1g, r1d, o32g, o32d, s2g, s2d, ryg, ryd, r2g, r2d,
     fg, fd, gfin, dfin, sqacc, sq, ld, wla, wcs, wcr, wxs, wxr, wys, wyr, was, war, wbs, wbr,
     s0s, s0r, s1s, s1r, sys, syr, s2s, s2r, s3s, s3r, s3ds, s3dr, sqs, sqr, osem) = scratch
    s, r = lax.axis_index("s"), lax.axis_index("r")
    xx, cc, yy = s // 2, s % 2, r // 4
    s1, s2, s3 = 2 * xx + 1 - cc, 2 * (1 - xx) + cc, 2 * (1 - xx) + 1 - cc
    across = (r + 4) % 8

    def remote(src, dst, send, recv, rr, ss):
        return pltpu.make_async_remote_copy(
            src_ref=src, dst_ref=dst, send_sem=send, recv_sem=recv, device_id={"r": rr, "s": ss}, device_id_type=MESH
        )

    barrier = pltpu.get_barrier_semaphore()
    for dr in (0, 4, 1, 7, 5, 3, 2, 6):
        for ds in range(4):
            if (dr, ds) != (0, 0):
                pl.semaphore_signal(barrier, inc=1, device_id={"r": (r + dr) % 8, "s": (s + ds) % 4}, device_id_type=MESH)

    WIDE = (512, 768)

    def first(part, x):
        return pl.multiple_of((1 - x) * 512, 256) if part else pl.multiple_of(x * 768, 256)

    def shard_in(j):
        return (wg_in, wu_in, wd_in)[j % 3].at[j // 3]

    def region(j, who):
        if j % 3 < 2:
            return wgu.at[j // 3, j % 3, pl.ds(aligned(who, DS), DS), :]
        return wd.at[j // 3, pl.ds(aligned(who, FS), FS), :]

    def own(j):
        return pltpu.make_async_copy(shard_in(j), region(j, s), wla.at[j])

    def to_core(j):
        return remote(region(j, s), region(j, s), wcs.at[j], wcr.at[j], r, s1)

    def half_of(j, who, half, x):
        if j in (2, 7):
            return wd.at[j // 7, pl.ds(aligned(2 * who + half, 160), 160), :]
        rows = pl.ds(aligned(2 * who + half, 64), 64)
        if j < 5:
            return wgu.at[0, j % 3 if j < 2 else j - 3, rows, pl.ds(first(j // 3, x), WIDE[j // 3])]
        return wgu.at[1, (j - 5) % 3, rows, slice(0, FC) if j < 7 else slice(FC, FF)]

    def by_x(j):
        return remote(half_of(j, s, yy, 1 - xx), half_of(j, s, yy, 1 - xx), wxs.at[j], wxr.at[j], r, s2)

    def by_y(j):
        return remote(half_of(j, s2, yy, xx), half_of(j, s2, yy, xx), wys.at[j], wyr.at[j], across, s)

    def by_core(j, half, send, recv):
        return remote(half_of(j, s2, half, xx), half_of(j, s2, half, xx), send.at[j], recv.at[j], r, s1)

    def got_x(j):
        by_x(j).wait_recv()
        by_y(j).start()
        by_core(j, yy, was, war).start()

    def got_y(j):
        by_y(j).wait_recv()
        by_core(j, 1 - yy, wbs, wbr).start()

    def got_core(j):
        by_core(j, yy, was, war).wait_recv()
        by_core(j, 1 - yy, wbs, wbr).wait_recv()

    sqacc[...] = jnp.zeros_like(sqacc)
    for j in range(6):
        own(j).start()
    load_x = pltpu.make_async_copy(x_in.at[0], hb, ld.at[0])
    load_dy = pltpu.make_async_copy(dy_in.at[0], dyb, ld.at[1])
    load_x.start()
    load_dy.start()
    for j in range(6):
        own(j).wait()
    pl.semaphore_wait(barrier, 31)
    for j in range(10):
        by_x(j).start()
    for j in range(6):
        to_core(j).start()
    load_x.wait()
    load_dy.wait()

    def prologue(i, _):
        rows = pl.ds(aligned(i, TB), TB)
        wide = hb[rows, :].astype(F32)
        a = (wide * norm_scale(wide)).astype(BF)
        a0[rows, :] = a
        a0t[:, rows] = a.T
        dyt[:, rows] = dyb[rows, :].T

        @pl.when(i == 6)
        def _():
            got_x(0)

        return 0

    lax.fori_loop(0, NT, prologue, 0)

    def mlp(a, start, width):
        o = None
        for c in range(width // FC):
            cols = pl.ds(pl.multiple_of(start + c * FC, FC), FC)
            g = dot(a, wgu[0, 0, :, cols])
            u = dot(a, wgu[0, 1, :, cols])
            p = (g * sigmoid(g) * u).astype(BF)
            one = dot(p, wd[0, cols, :])
            o = one if o is None else o + one
        return o

    def fwd_first(i, _):
        @pl.when(i == 2)
        def _():
            got_x(3)

        @pl.when(i == 5)
        def _():
            got_x(4)

        rows = pl.ds(aligned(i, TB), TB)
        da[rows, :] = mlp(a0[rows, :], first(0, xx), WIDE[0])
        return 0

    def fwd_second(i, _):
        @pl.when(i == 0)
        def _():
            got_x(5)
            got_x(6)

        @pl.when(i == 1)
        def _():
            got_x(7)

        @pl.when(i == 2)
        def _():
            got_y(5)
            got_y(6)

        @pl.when(i == 3)
        def _():
            got_x(8)

        @pl.when(i == 5)
        def _():
            got_x(9)
            got_y(7)

        rows = pl.ds(aligned(i, TB), TB)
        o = da[rows, :] + mlp(a0[rows, :], first(1, xx), WIDE[1])
        da[rows, :] = jnp.zeros((TB, D), F32)
        h = hb[rows, :] + o.astype(BF)
        hb[rows, :] = h
        wide = h.astype(F32)
        a = (wide * norm_scale(wide)).astype(BF)
        a1[rows, :] = a
        a1t[:, rows] = a.T
        return 0

    got_x(1)
    got_y(0)
    got_y(1)
    got_x(2)
    for j in range(3):
        to_core(j).wait_recv()
    got_core(0)
    got_core(1)
    lax.fori_loop(0, NT, fwd_first, 0)
    for j in (2, 3, 4):
        got_y(j)
    for j in (2, 3, 4):
        got_core(j)
    lax.fori_loop(0, NT, fwd_second, 0)
    for j in range(3, 6):
        to_core(j).wait_recv()
    for j in (5, 6, 7):
        got_core(j)

    def part(m, who):
        return pl.ds(aligned(who, 64), 64) if m == 2 else pl.ds(aligned(who, DS), DS)

    def mine(m, gu, d):
        return (lambda g, *at: d.at[(g, *at)]) if m == 2 else (lambda g, *at: gu.at[(g, m, *at)])

    def stage0(g, m, w):
        slot = g % 2
        src = mine(m, sbg, sbd)(slot, part(m, (s1, s3)[w]), slice(None))
        return remote(src, mine(m, r0g, r0d)(slot, w), s0s.at[slot, m // 2], s0r.at[slot, 2 * m + w], r, s1)

    def stage0_sent(g):
        slot = g % 2
        pltpu.make_async_copy(r0g.at[slot], r0g.at[slot], s0s.at[slot, 0]).wait()
        pltpu.make_async_copy(r0d.at[slot], r0d.at[slot], s0s.at[slot, 1]).wait()

    def stage1(g, m):
        return remote(mine(m, t1g, t1d)(g % 2), mine(m, r1g, r1d)(g), s1s.at[g % 2, m], s1r.at[g, m], r, s2)

    def piece(m, who):
        if m == 2:
            return pl.ds(aligned(who // 2, 16), 16), pl.ds(aligned(who % 2, 256), 256)
        return pl.ds(aligned(who, 16), 16), slice(None)

    def half(m, y):
        return pl.ds(aligned(y, 32), 32) if m == 2 else pl.ds(aligned(y, 64), 64)

    def stage2y(g, m):
        return remote(
            mine(m, s2g, s2d)(g, half(m, 1 - yy), slice(None)), mine(m, ryg, ryd)(g), sys.at[m // 2], syr.at[g, m], across, s
        )

    def stage2(g, m, k):
        to = 4 * yy + (r % 4 + k) % 4
        return remote(
            mine(m, s2g, s2d)(g, *piece(m, to)), mine(m, r2g, r2d)(g, k - 1), s2s.at[m // 2], s2r.at[g, 3 * m + k - 1], to, s
        )

    def place(g):
        block = 4 * (g % NC) + s
        spot = pl.ds(aligned(4 * (block % 5) + r // 2, 16), 16), pl.ds(aligned(r % 2, 256), 256)
        return 1 - g // NC, g % NC, block // 5, spot

    def stage3(g, m, k):
        to = (r + k) % 8
        layer, c, owner, spot = place(g)
        if m == 2:
            return remote(fd.at[g], dfin.at[(layer, *spot)], s3ds, s3dr, to, owner)
        return remote(fg.at[g, m], gfin.at[layer, m, pl.ds(aligned(r, 16), 16), pl.ds(aligned(c, FC), FC)], s3s, s3r, to, s)

    def add0(g, m, fresh):
        slot = g % 2
        for w in (1, 0):
            stage0(g, m, w).wait_recv()
        if not fresh:
            stage1(g, m).wait_send()
        own_term = mine(m, sbg, sbd)
        arrived = mine(m, r0g, r0d)
        other = own_term(slot, part(m, s2), slice(None))[...].astype(F32) + arrived(slot, 1)[...].astype(F32)
        mine(m, t1g, t1d)(slot)[...] = other.astype(BF)
        stage1(g, m).start()
        kept = own_term(slot, part(m, s), slice(None))[...].astype(F32) + arrived(slot, 0)[...].astype(F32)
        mine(m, o32g, o32d)(g % 4)[...] = kept

    def add1(g, m):
        stage1(g, m).wait_recv()
        total = mine(m, o32g, o32d)(g % 4)[...] + mine(m, r1g, r1d)(g)[...].astype(F32)
        mine(m, o32g, o32d)(g % 4)[...] = total
        mine(m, s2g, s2d)(g)[...] = total.astype(BF)
        stage2y(g, m).start()

    def add2y(g, m):
        stage2y(g, m).wait_recv()
        here = half(m, yy), slice(None)
        total = mine(m, o32g, o32d)(g % 4, *here)[...] + mine(m, ryg, ryd)(g)[...].astype(F32)
        mine(m, o32g, o32d)(g % 4, *here)[...] = total
        mine(m, s2g, s2d)(g, *here)[...] = total.astype(BF)
        for k in (2, 3, 1):
            stage2(g, m, k).start()

    def add2(g, m):
        for k in range(1, 4):
            stage2(g, m, k).wait_recv()
        total = mine(m, o32g, o32d)(g % 4, *piece(m, r))[...]
        for k in range(3):
            total += mine(m, r2g, r2d)(g, k)[...].astype(F32)
        total = total.astype(BF)
        mine(m, fg, fd)(g)[...] = total
        square = total.astype(F32)
        square = square * square
        sqacc[...] += (square[:8, :128] + square[:8, 128:]) + (square[8:, :128] + square[8:, 128:])
        layer, c, owner, spot = place(g)
        if m == 2:

            @pl.when(owner == s)
            def _():
                dfin[(layer, *spot)] = total

            @pl.when(owner != s)
            def _():
                stage3(g, m, 0).start()
        else:
            gfin[layer, m, pl.ds(aligned(r, 16), 16), pl.ds(aligned(c, FC), FC)] = total
        for k in (4, 5, 3, 6, 2, 7, 1):
            stage3(g, m, k).start()

    def backward(layer, a_ref, at_ref, with_da):
        def chunk(c, _):
            cols = pl.ds(aligned(c, FC), FC)
            n = (1 - layer) * NC + c

            def block(i, _):
                @pl.when((i == 0) & (n >= 2))
                def _():
                    for m in range(3):
                        add1(n - 2, m)

                @pl.when((i == 1) & (n >= 3))
                def _():
                    for m in range(3):
                        add0(n - 1, m, False)
                        add2(n - 3, m)

                @pl.when((i == 1) & (n >= 1) & (n < 3))
                def _():
                    for m in range(3):
                        add0(n - 1, m, True)

                @pl.when((i == 2) & (n >= 2))
                def _():
                    for m in range(3):
                        add2y(n - 2, m)

                if with_da:

                    @pl.when((i == 1) & (n == 0))
                    def _():
                        got_y(8)

                    @pl.when((i == 2) & (n == 0))
                    def _():
                        got_y(9)

                    @pl.when((i == 3) & (n == 0))
                    def _():
                        got_core(8)
                        got_core(9)

                def rows(q):
                    return pl.ds(aligned(i * (TBB // SB) + q, SB), SB)

                def front(q):
                    a = a_ref[rows(q), :]
                    g = dot(a, wgu[layer, 0, :, cols])
                    u = dot(a, wgu[layer, 1, :, cols])
                    dp = dot_t(dyb[rows(q), :], wd[layer, cols, :]).astype(BF).astype(F32)
                    sig = sigmoid(g)
                    sl = g * sig
                    dsl = sig + sl * (1.0 - sig)
                    return (dp * u * dsl).astype(BF), (dp * sl).astype(BF), (sl * u).astype(BF)

                def back(qs, of):
                    for m, left in enumerate((at_ref, at_ref, dyt)):
                        base = jnp.where(i > 0, acc[m], 0.0) if qs[0] == 0 else acc[m]
                        acc[m] = base + sum(dot(left[:, rows(q)], of[q][m]) for q in qs)
                    if with_da:
                        for q in qs:
                            da[rows(q), :] += dot_t(of[q][0], wgu[layer, 0, :, cols]) + dot_t(of[q][1], wgu[layer, 1, :, cols])

                of = [front(q) for q in range(4)]
                back((0, 1, 2, 3), of)
                return 0

            lax.fori_loop(0, BB, block, 0)
            slot = n % 2

            @pl.when(n >= 2)
            def _():
                stage0_sent(n)

            for m in range(3):
                mine(m, sbg, sbd)(slot)[...] = (acc[m].T if m == 2 else acc[m]).astype(BF)
                for w in (1, 0):
                    stage0(n, m, w).start()
            return 0

        lax.fori_loop(0, NC, chunk, 0)

    backward(1, a1, a1t, True)

    def norm_back(i, _):
        rows = pl.ds(aligned(i, TB), TB)
        wide = hb[rows, :].astype(F32)
        scale = norm_scale(wide)
        t = da[rows, :].astype(BF).astype(F32)
        back = scale * t - wide * (scale * scale * scale * jnp.mean(t * wide, -1, keepdims=True))
        dh = dyb[rows, :] + back.astype(BF)
        dyb[rows, :] = dh
        dyt[:, rows] = dh.T
        return 0

    lax.fori_loop(0, NT, norm_back, 0)
    backward(0, a0, a0t, False)

    for which, g in ((add1, G - 2), (add2, G - 3), (functools.partial(add0, fresh=False), G - 1), (add2y, G - 2), (add1, G - 1),
                     (add2, G - 2), (add2y, G - 1), (add2, G - 1)):
        for m in range(3):
            which(g, m)

    me = 4 * r + s
    sq[me] = sqacc[...]
    for dr in range(8):
        for ds in range(4):
            if (dr, ds) != (0, 0):
                remote(sq.at[me], sq.at[me], sqs, sqr, (r + dr) % 8, (s + ds) % 4).start()

    def bytes_of(ref, sem):
        pltpu.make_async_copy(ref, ref, sem).wait()

    bytes_of(gfin.at[:, :, 0 : 7 * 16, :], s3r)
    bytes_of(dfin.at[:, 0:304, :], s3dr)
    out_g = pltpu.make_async_copy(gfin, gu_out, osem.at[0])
    out_d = pltpu.make_async_copy(dfin, d_out, osem.at[1])
    out_g.start()
    out_d.start()

    bytes_of(sq.at[0:31], sqr)
    total = sq[0]
    for j in range(1, 32):
        total += sq[j]
    sq_out[...] = total
    for j in range(6):
        to_core(j).wait_send()
    for j in range(10):
        by_x(j).wait_send()
        by_y(j).wait_send()
        by_core(j, yy, was, war).wait_send()
        by_core(j, 1 - yy, wbs, wbr).wait_send()
    stage0_sent(G - 2)
    stage0_sent(G - 1)
    for m in range(3):
        stage1(G - 2, m).wait_send()
        stage1(G - 1, m).wait_send()
    bytes_of(ryg, sys.at[0])
    bytes_of(ryd, sys.at[1])
    bytes_of(r2g, s2s.at[0])
    bytes_of(r2d, s2s.at[1])
    bytes_of(gfin.at[:, :, 0 : 7 * 16, :], s3s)
    bytes_of(dfin.at[:, 0:304, :], s3ds)
    bytes_of(sq.at[0:31], sqs)
    out_g.wait()
    out_d.wait()


def optimizer(sq_ref, *refs):
    count = 4 * L * (2 * DS * FF + FS * D)
    factor = jnp.minimum(1.0, 0.5 * lax.rsqrt(jnp.sum(sq_ref[...], keepdims=True) / count + 1e-30))
    for i in range(3):
        g, w, m, v = (refs[3 * which + i] for which in range(4))
        g = g[...].reshape(w.shape).astype(F32) * factor.reshape(1, 1, 1)
        new_m = 0.9 * m[...] + 0.1 * g
        new_v = 0.95 * v[...] + 0.05 * g * g
        step = new_m * lax.rsqrt(new_v + 1e-8) + 0.1 * w[...].astype(F32)
        refs[12 + i][...] = (w[...].astype(F32) - 0.02 * step).astype(BF)
        refs[15 + i][...] = new_m
        refs[18 + i][...] = new_v


def solution(mesh):
    def step(x, dy, *arrays):
        weights, ms, vs = (arrays[i : i + 3] for i in (0, 3, 6))
        hbm = pl.BlockSpec(memory_space=pl.ANY)
        dma = pltpu.SemaphoreType.DMA
        gu, d, sq = pl.pallas_call(
            kernel,
            name="train_step",
            out_shape=(
                jax.ShapeDtypeStruct((L, 2, DS, FF), BF),
                jax.ShapeDtypeStruct((L, FS, D), BF),
                jax.ShapeDtypeStruct((8, 128), F32),
            ),
            in_specs=[hbm] * 5,
            out_specs=(hbm, hbm, pl.BlockSpec(memory_space=pltpu.VMEM)),
            scratch_shapes=[
                pltpu.VMEM((T, D), BF),
                pltpu.VMEM((T, D), BF),
                pltpu.VMEM((T, D), BF),
                pltpu.VMEM((T, D), BF),
                pltpu.VMEM((D, T), BF),
                pltpu.VMEM((D, T), BF),
                pltpu.VMEM((D, T), BF),
                pltpu.VMEM((T, D), F32),
                pltpu.VMEM((L, 2, D, FF), BF),
                pltpu.VMEM((L, FF, D), BF),
                pltpu.VMEM((3, D, FC), F32),
                pltpu.VMEM((2, 2, D, FC), BF),
                pltpu.VMEM((2, FC, D), BF),
                pltpu.VMEM((2, 2, 2, DS, FC), BF),
                pltpu.VMEM((2, 2, FC // 4, D), BF),
                pltpu.VMEM((2, 2, DS, FC), BF),
                pltpu.VMEM((2, FC // 4, D), BF),
                pltpu.VMEM((G, 2, DS, FC), BF),
                pltpu.VMEM((G, FC // 4, D), BF),
                pltpu.VMEM((4, 2, DS, FC), F32),
                pltpu.VMEM((4, FC // 4, D), F32),
                pltpu.VMEM((G, 2, DS, FC), BF),
                pltpu.VMEM((G, FC // 4, D), BF),
                pltpu.VMEM((G, 2, DS // 2, FC), BF),
                pltpu.VMEM((G, FC // 8, D), BF),
                pltpu.VMEM((G, 2, 3, 16, FC), BF),
                pltpu.VMEM((G, 3, 16, 256), BF),
                pltpu.VMEM((G, 2, 16, FC), BF),
                pltpu.VMEM((G, 16, 256), BF),
                pltpu.VMEM((L, 2, DS, FF), BF),
                pltpu.VMEM((L, FS, D), BF),
                pltpu.VMEM((8, 128), F32),
                pltpu.VMEM((32, 8, 128), F32),
                dma((2,)),
                dma((6,)), dma((6,)), dma((6,)),
                dma((10,)), dma((10,)), dma((10,)), dma((10,)), dma((10,)), dma((10,)), dma((10,)), dma((10,)),
                dma((2, 2)), dma((2, 6)), dma((2, 3)), dma((G, 3)),
                dma((2,)), dma((G, 3)), dma((2,)), dma((G, 9)),
                dma(()), dma(()), dma(()), dma(()),
                dma(()), dma(()), dma((2,)),
            ],
            compiler_params=pltpu.CompilerParams(collective_id=0, has_side_effects=True, vmem_limit_bytes=67043328),
        )(x, dy, *weights)
        wide = pl.BlockSpec((1, DS // STEPS, FF), lambda l, i: (l, i, 0))
        deep = pl.BlockSpec((1, FS // STEPS, D), lambda l, i: (l, i, 0))
        three = [wide, wide, deep]
        gate = pl.BlockSpec((1, 1, DS // STEPS, FF), lambda l, i: (l, 0, i, 0))
        up = pl.BlockSpec((1, 1, DS // STEPS, FF), lambda l, i: (l, 1, i, 0))
        new = pl.pallas_call(
            optimizer,
            name="optimizer",
            grid=(L, STEPS),
            out_shape=[jax.ShapeDtypeStruct(a.shape, t) for t, which in ((BF, weights), (F32, ms), (F32, vs)) for a in which],
            in_specs=[pl.BlockSpec((8, 128), lambda l, i: (0, 0)), gate, up, deep] + three * 3,
            out_specs=three * 3,
            compiler_params=pltpu.CompilerParams(dimension_semantics=("arbitrary", "arbitrary")),
        )(sq, gu, gu, d, *weights, *ms, *vs)
        return tuple(new)

    states, cut = P(("rep", "r", "s"), None, None), P(None, "s", None)
    return jax.shard_map(
        step, mesh=mesh, in_specs=(states, states) + (cut,) * 9, out_specs=(P("rep", "s", None),) * 9, check_vma=False
    )
```

```python
import jax
import jax.numpy as jnp
from jax import lax
from jax.experimental import pallas as pl
from jax.experimental.pallas import tpu as pltpu
from jax.sharding import PartitionSpec as P

MESH = pl.DeviceIdType.MESH
BF, F32 = jnp.bfloat16, jnp.float32
ALL, MATRICES, OTHERS, BOTH = slice(None), range(3), range(1, 32), (1, 0)
T, D, FF, L = 4096, 512, 1280, 2
TB, FC = 512, 256
NT, NC = T // TB, FF // FC
TBB, SB = 1024, 256
BB = T // TBB
G = L * NC
STEPS = 1
DS, FS = D // 4, FF // 4
QR, GU = FC // 4, (2, DS, FC)


def dot(a, b):
    return jnp.dot(a, b, preferred_element_type=F32)


def dot_t(a, b):
    return lax.dot_general(a, b, (((1,), (1,)), ((), ())), preferred_element_type=F32)


def sigmoid(g):
    return 0.5 + 0.5 * jnp.tanh(0.5 * g)


def norm_scale(wide):
    return lax.rsqrt(jnp.mean(wide * wide, -1, keepdims=True) + 1e-6)


def aligned(i, n):
    return pl.multiple_of(i * n, n)


def kernel(x_in, dy_in, wg_in, wu_in, wd_in, gu_out, d_out, sq_out, kept, *scratch):
    (hb, dyb, a0, a1, at, dyt, da, wgu, wd, acc, sbg, sbd, r0g, r0d, t1g, t1d, r1g, r1d, o32g, o32d, s2g, s2d, ryg, ryd, r2g, r2d,
     fg, fd, gfin, dfin, sqacc, sq, st, sts, ks, ld, wla, wcs, wcr, wxs, wxr, wys, wyr, was, war, wbs, wbr,
     s0s, s0r, s1s, s1r, sys, syr, s2s, s2r, s3s, s3r, s3ys, s3yr, s3ds, s3dr, sqs, sqr, osem) = scratch
    s, r = lax.axis_index("s"), lax.axis_index("r")
    xx, cc, yy = s // 2, s % 2, r // 4
    s1, s2 = s + 1 - 2 * cc, (s + 2) % 4
    s3 = (s1 + 2) % 4
    across = (r + 4) % 8

    def other(k):
        return {"r": (r + k // 4) % 8, "s": (s + k) % 4}

    def remote(src, dst, send, recv, rr, ss):
        return pltpu.make_async_remote_copy(
            src_ref=src, dst_ref=dst, send_sem=send, recv_sem=recv, device_id={"r": rr, "s": ss}, device_id_type=MESH
        )

    barrier = pltpu.get_barrier_semaphore()
    for k in OTHERS:
        pl.semaphore_signal(barrier, inc=1, device_id=other(k), device_id_type=MESH)

    WIDE = (512, 768)

    def first(part, x):
        return pl.multiple_of((1 - x) * 512, 256) if part else pl.multiple_of(x * 768, 256)

    def shard_in(j):
        return (wg_in, wu_in, wd_in)[j % 3].at[j // 3]

    def region(j, who):
        if j % 3 < 2:
            return wgu.at[j // 3, j % 3, pl.ds(aligned(who, DS), DS), :]
        return wd.at[j // 3, pl.ds(aligned(who, FS), FS), :]

    def own(j):
        return pltpu.make_async_copy(shard_in(j), region(j, s), wla.at[j])

    def to_core(j):
        return remote(region(j, s), region(j, s), wcs.at[j], wcr.at[j], r, s1)

    def half_of(j, who, half, x):
        if j in (2, 7):
            return wd.at[j // 7, pl.ds(aligned(2 * who + half, 160), 160), :]
        rows = pl.ds(aligned(2 * who + half, 64), 64)
        if j < 5:
            return wgu.at[0, j % 3 if j < 2 else j - 3, rows, pl.ds(first(j // 3, x), WIDE[j // 3])]
        return wgu.at[1, (j - 5) % 3, rows, slice(0, FC) if j < 7 else slice(FC, FF)]

    def by_x(j):
        return remote(half_of(j, s, yy, 1 - xx), half_of(j, s, yy, 1 - xx), wxs.at[j], wxr.at[j], r, s2)

    def by_y(j):
        return remote(half_of(j, s2, yy, xx), half_of(j, s2, yy, xx), wys.at[j], wyr.at[j], across, s)

    def by_core(j, half, send, recv):
        return remote(half_of(j, s2, half, xx), half_of(j, s2, half, xx), send.at[j], recv.at[j], r, s1)

    def got_x(j):
        by_x(j).wait_recv()
        by_y(j).start()
        by_core(j, yy, was, war).start()

    def got_y(j):
        by_y(j).wait_recv()
        by_core(j, 1 - yy, wbs, wbr).start()

    def got_core(j):
        by_core(j, yy, was, war).wait_recv()
        by_core(j, 1 - yy, wbs, wbr).wait_recv()

    sqacc[...] = jnp.zeros_like(sqacc)
    for j in range(6):
        own(j).start()
    load_x = pltpu.make_async_copy(x_in.at[0], hb, ld.at[0])
    load_dy = pltpu.make_async_copy(dy_in.at[0], dyb, ld.at[1])
    load_x.start()
    load_dy.start()
    for j in range(6):
        own(j).wait()
    pl.semaphore_wait(barrier, 31)
    for j in range(10):
        by_x(j).start()
    for j in range(6):
        to_core(j).start()
    load_x.wait()
    load_dy.wait()

    def prologue(i, _):
        rows = pl.ds(aligned(i, TB), TB)
        wide = hb[rows, :].astype(F32)
        a = (wide * norm_scale(wide)).astype(BF)
        a0[rows, :] = a
        dyt[:, rows] = dyb[rows, :].T

        @pl.when(i == 6)
        def _():
            got_x(0)

        return 0

    lax.fori_loop(0, NT, prologue, 0)

    def mlp(a, start, width, slot):
        o = None
        for c in range(width // FC):
            cols = pl.ds(pl.multiple_of(start + c * FC, FC), FC)
            g = dot(a, wgu[0, 0, :, cols])
            u = dot(a, wgu[0, 1, :, cols])
            st[slot, c, :, :FC] = g
            st[slot, c, :, FC:] = u
            p = (g * sigmoid(g) * u).astype(BF)
            one = dot(p, wd[0, cols, :])
            o = one if o is None else o + one
        return o

    def keep(i, part):
        slot, count = i % 2, WIDE[part] // FC
        return pltpu.make_async_copy(
            st.at[slot, :count],
            kept.at[pl.ds(first(part, xx) // FC, count), pl.ds(aligned(i, TB), TB), :],
            sts.at[slot],
        )

    def free_slot(i, part):
        @pl.when(i >= 2)
        def _():
            keep(i, part).wait()

    def fwd_first(i, _):
        @pl.when(i == 2)
        def _():
            got_x(3)

        @pl.when(i == 5)
        def _():
            got_x(4)

        free_slot(i, 0)
        rows = pl.ds(aligned(i, TB), TB)
        da[rows, :] = mlp(a0[rows, :], first(0, xx), WIDE[0], i % 2)
        keep(i, 0).start()
        return 0

    def fwd_second(i, _):
        @pl.when(i == 0)
        def _():
            for j in (5, 6):
                got_x(j)

        @pl.when(i == 1)
        def _():
            got_x(7)

        @pl.when(i == 2)
        def _():
            got_y(5)
            got_y(6)

        @pl.when(i == 3)
        def _():
            got_x(8)

        @pl.when(i == 5)
        def _():
            got_x(9)
            got_y(7)

        free_slot(i, 1)
        rows = pl.ds(aligned(i, TB), TB)
        o = da[rows, :] + mlp(a0[rows, :], first(1, xx), WIDE[1], i % 2)
        keep(i, 1).start()
        da[rows, :] = jnp.zeros((TB, D), F32)
        h = hb[rows, :] + o.astype(BF)
        hb[rows, :] = h
        wide = h.astype(F32)
        a = (wide * norm_scale(wide)).astype(BF)
        a1[rows, :] = a
        at[:, rows] = a.T
        return 0

    got_x(1)
    got_y(0)
    got_y(1)
    got_x(2)
    for j in MATRICES:
        to_core(j).wait_recv()
    got_core(0)
    got_core(1)
    lax.fori_loop(0, NT, fwd_first, 0)
    keep(NT - 2, 0).wait()
    keep(NT - 1, 0).wait()
    for get in (got_y, got_core):
        for j in (2, 3, 4):
            get(j)
    lax.fori_loop(0, NT, fwd_second, 0)
    keep(NT - 2, 1).wait()
    keep(NT - 1, 1).wait()
    for j in range(3, 6):
        to_core(j).wait_recv()
    for j in (5, 6, 7):
        got_core(j)

    def part(m, who):
        return pl.ds(aligned(who, 64), 64) if m == 2 else pl.ds(aligned(who, DS), DS)

    def mine(m, gu, d):
        return (lambda g, *at: d.at[(g, *at)]) if m == 2 else (lambda g, *at: gu.at[(g, m, *at)])

    def stage0(g, m, w):
        slot = g % 2
        src = mine(m, sbg, sbd)(slot, part(m, (s1, s3)[w]), ALL)
        return remote(src, mine(m, r0g, r0d)(slot, w), s0s.at[slot, m // 2], s0r.at[slot, 2 * m + w], r, s1)

    def stage0_sent(g):
        slot = g % 2
        pltpu.make_async_copy(r0g.at[slot], r0g.at[slot], s0s.at[slot, 0]).wait()
        pltpu.make_async_copy(r0d.at[slot], r0d.at[slot], s0s.at[slot, 1]).wait()

    def stage1(g, m):
        return remote(mine(m, t1g, t1d)(g), mine(m, r1g, r1d)(g), s1s.at[m // 2], s1r.at[g, m], r, s2)

    def piece(m, who):
        if m == 2:
            return pl.ds(aligned(who // 2, 16), 16), pl.ds(aligned(who % 2, 256), 256)
        return pl.ds(aligned(who, 16), 16), ALL

    def half(m, y):
        return pl.ds(aligned(y, 32), 32) if m == 2 else pl.ds(aligned(y, 64), 64)

    def stage2y(g, m):
        return remote(
            mine(m, s2g, s2d)(g, half(m, 1 - yy), ALL), mine(m, ryg, ryd)(g), sys.at[m // 2], syr.at[g, m], across, s
        )

    def stage2(g, m, k):
        to = 4 * yy + (r % 4 + k) % 4
        return remote(
            mine(m, s2g, s2d)(g, *piece(m, to)), mine(m, r2g, r2d)(g, k - 1), s2s.at[m // 2], s2r.at[g, 3 * m + k - 1], to, s
        )

    def place(g):
        block = 4 * (g % NC) + s
        spot = pl.ds(aligned(4 * (block % 5) + r // 2, 16), 16), pl.ds(aligned(r % 2, 256), 256)
        return 1 - g // NC, g % NC, block // 5, spot

    def stage3(g, m, k):
        layer, c, owner, spot = place(g)
        if m == 2:
            return remote(fd.at[g], dfin.at[(layer, *spot)], s3ds, s3dr, (r + k) % 8, owner)
        to = 4 * yy + (r % 4 + k) % 4
        where = gfin.at[layer, m, pl.ds(aligned(r, 16), 16), pl.ds(aligned(c, FC), FC)]
        return remote(fg.at[g, m], where, s3s, s3r.at[g, m], to, s)

    def stage3y(g, m):
        layer, c, _, _ = place(g)
        block = gfin.at[layer, m, pl.ds(aligned(yy, 64), 64), pl.ds(aligned(c, FC), FC)]
        return remote(block, block, s3ys, s3yr, across, s)

    def add3(g, m):
        if m < 2:
            pltpu.make_async_copy(r2g.at[g, m], r2g.at[g, m], s3r.at[g, m]).wait()
            stage3y(g, m).start()

    def add0(g, m):
        slot = g % 2
        for w in BOTH:
            stage0(g, m, w).wait_recv()
        own_term = mine(m, sbg, sbd)
        arrived = mine(m, r0g, r0d)
        other = own_term(slot, part(m, s2), ALL)[...].astype(F32) + arrived(slot, 1)[...].astype(F32)
        mine(m, t1g, t1d)(g)[...] = other.astype(BF)
        stage1(g, m).start()
        kept = own_term(slot, part(m, s), ALL)[...].astype(F32) + arrived(slot, 0)[...].astype(F32)
        mine(m, o32g, o32d)(g % 4)[...] = kept

    def add1(g, m):
        stage1(g, m).wait_recv()
        total = mine(m, o32g, o32d)(g % 4)[...] + mine(m, r1g, r1d)(g)[...].astype(F32)
        mine(m, o32g, o32d)(g % 4)[...] = total
        mine(m, s2g, s2d)(g)[...] = total.astype(BF)
        stage2y(g, m).start()

    def add2y(g, m):
        stage2y(g, m).wait_recv()
        here = half(m, yy), ALL
        total = mine(m, o32g, o32d)(g % 4, *here)[...] + mine(m, ryg, ryd)(g)[...].astype(F32)
        mine(m, o32g, o32d)(g % 4, *here)[...] = total
        mine(m, s2g, s2d)(g, *here)[...] = total.astype(BF)
        for k in range(3, 0, -1):
            stage2(g, m, k).start()

    def add2(g, m):
        for k in range(1, 4):
            stage2(g, m, k).wait_recv()
        total = mine(m, o32g, o32d)(g % 4, *piece(m, r))[...]
        for k in MATRICES:
            total += mine(m, r2g, r2d)(g, k)[...].astype(F32)
        total = total.astype(BF)
        mine(m, fg, fd)(g)[...] = total
        square = total.astype(F32)
        square = square * square
        sqacc[...] += square[:8, :128] + square[:8, 128:] + square[8:, :128] + square[8:, 128:]
        layer, c, owner, spot = place(g)
        if m == 2:

            @pl.when(owner == s)
            def _():
                dfin[(layer, *spot)] = total

            @pl.when(owner != s)
            def _():
                stage3(g, m, 0).start()
        else:
            gfin[layer, m, pl.ds(aligned(r, 16), 16), pl.ds(aligned(c, FC), FC)] = total
        for k in range(7 if m == 2 else 3, 0, -1):
            stage3(g, m, k).start()

    def recall(c, at_row, count):
        rows = pl.ds(pl.multiple_of(at_row, TB), count)
        return pltpu.make_async_copy(kept.at[c, rows, :], da.at[rows, :], ks.at[at_row // TBB])

    def backward(layer, with_da):
        def chunk(c, _):
            cols = pl.ds(aligned(c, FC), FC)
            n = (1 - layer) * NC + c

            def block(i, _):
                @pl.when((i == 0) & (n >= 2))
                def _():
                    for m in MATRICES:
                        add1(n - 2, m)

                @pl.when((i == 1) & (n >= 4))
                def _():
                    for m in range(2):
                        add3(n - 4, m)

                @pl.when((i == 1) & (n >= 1))
                def _():
                    for m in MATRICES:
                        add0(n - 1, m)

                @pl.when((i == 2) & (n >= 3))
                def _():
                    for m in MATRICES:
                        add2(n - 3, m)

                @pl.when((i == 3) & (n >= 2))
                def _():
                    for m in MATRICES:
                        add2y(n - 2, m)

                if with_da:

                    @pl.when((i == 1) & (n == 0))
                    def _():
                        got_y(8)

                    @pl.when((i == 2) & (n == 0))
                    def _():
                        got_y(9)

                    @pl.when((i == 3) & (n == 0))
                    def _():
                        got_core(8)
                        got_core(9)

                if not with_da:
                    recall(c, i * TBB, TBB).wait()

                def rows(q):
                    return pl.ds(aligned(i * (TBB // SB) + q, SB), SB)

                def front(q):
                    if with_da:
                        a = a1[rows(q), :]
                        g = dot(a, wgu[layer, 0, :, cols])
                        u = dot(a, wgu[layer, 1, :, cols])
                    else:
                        g, u = da[rows(q), :FC], da[rows(q), FC:]
                    dp = dot_t(dyb[rows(q), :], wd[layer, cols, :]).astype(BF).astype(F32)
                    sig = sigmoid(g)
                    sl = g * sig
                    dsl = sig + sl * (1.0 - sig)
                    return (dp * u * dsl).astype(BF), (dp * sl).astype(BF), (sl * u).astype(BF)

                def back(qs, of):
                    for m, left in enumerate((at, at, dyt)):
                        base = jnp.where(i > 0, acc[m], 0.0) if qs[0] == 0 else acc[m]
                        acc[m] = base + sum(dot(left[:, rows(q)], of[q][m]) for q in qs)
                    if with_da:
                        for q in qs:
                            da[rows(q), :] += dot_t(of[q][0], wgu[layer, 0, :, cols]) + dot_t(of[q][1], wgu[layer, 1, :, cols])

                if with_da:
                    of = [front(q) for q in range(4)]
                    back((0, 1, 2, 3), of)
                else:
                    of = [front(q) for q in range(4)]
                    back((0, 1), of)
                    back((2, 3), of)
                if not with_da:

                    @pl.when(c < NC - 1)
                    def _():
                        recall(c + 1, i * TBB, TBB).start()

                return 0

            lax.fori_loop(0, BB, block, 0)
            slot = n % 2

            @pl.when(n >= 2)
            def _():
                stage0_sent(n)

            for m in MATRICES:
                mine(m, sbg, sbd)(slot)[...] = (acc[m].T if m == 2 else acc[m]).astype(BF)
                for w in BOTH:
                    stage0(n, m, w).start()
            return 0

        lax.fori_loop(0, NC, chunk, 0)

    backward(1, True)

    def norm_back(i, _):
        rows = pl.ds(aligned(i, TB), TB)
        wide = hb[rows, :].astype(F32)
        scale = norm_scale(wide)
        t = da[rows, :].astype(BF).astype(F32)
        back = scale * t - wide * (scale * scale * scale * jnp.mean(t * wide, -1, keepdims=True))
        dh = dyb[rows, :] + back.astype(BF)
        dyb[rows, :] = dh
        dyt[:, rows] = dh.T
        at[:, rows] = a0[rows, :].T
        recall(0, i * TB, TB).start()
        return 0

    lax.fori_loop(0, NT, norm_back, 0)
    backward(0, False)

    for which, g in ((add1, G - 2), (add3, G - 4), (add2, G - 3), (add0, G - 1), (add2y, G - 2), (add1, G - 1), (add3, G - 3),
                     (add2y, G - 1), (add2, G - 2), (add2, G - 1)):
        for m in MATRICES:
            which(g, m)

    me = 4 * r + s
    sq[me] = sqacc[...]
    for k in OTHERS:
        remote(sq.at[me], sq.at[me], sqs, sqr, *other(k).values()).start()

    def bytes_of(ref, sem):
        pltpu.make_async_copy(ref, ref, sem).wait()

    for g in (G - 2, G - 1):
        for m in range(2):
            add3(g, m)
    bytes_of(gfin.at[:, :, :64], s3yr)
    bytes_of(dfin.at[:, :304], s3dr)
    out_g = pltpu.make_async_copy(gfin, gu_out, osem.at[0])
    out_d = pltpu.make_async_copy(dfin, d_out, osem.at[1])
    out_g.start()
    out_d.start()

    bytes_of(sq.at[:31], sqr)
    total = sq[0]
    for j in range(1, 32):
        total += sq[j]
    sq_out[...] = total
    for j in range(6):
        to_core(j).wait_send()
    for j in range(10):
        by_x(j).wait_send()
        by_y(j).wait_send()
        by_core(j, yy, was, war).wait_send()
        by_core(j, 1 - yy, wbs, wbr).wait_send()
    stage0_sent(G - 2)
    stage0_sent(G - 1)
    bytes_of(t1g, s1s.at[0])
    bytes_of(t1d, s1s.at[1])
    bytes_of(ryg, sys.at[0])
    bytes_of(ryd, sys.at[1])
    bytes_of(r2g, s2s.at[0])
    bytes_of(r2d, s2s.at[1])
    bytes_of(r2g, s3s)
    bytes_of(gfin.at[:, :, :64], s3ys)
    bytes_of(dfin.at[:, :304], s3ds)
    bytes_of(sq.at[:31], sqs)
    out_g.wait()
    out_d.wait()


def optimizer(sq_ref, *refs):
    count = 4 * L * (2 * DS * FF + FS * D)
    factor = jnp.minimum(1.0, 0.5 * lax.rsqrt(jnp.sum(sq_ref[...], keepdims=True) / count + 1e-30))
    for i in MATRICES:
        g, w, m, v = (refs[3 * which + i] for which in range(4))
        g = g[...].reshape(w.shape).astype(F32) * factor.reshape(1, 1, 1)
        new_m = 0.9 * m[...] + 0.1 * g
        new_v = 0.95 * v[...] + 0.05 * g * g
        step = new_m * lax.rsqrt(new_v + 1e-8) + 0.1 * w[...].astype(F32)
        refs[12 + i][...] = (w[...].astype(F32) - 0.02 * step).astype(BF)
        refs[15 + i][...] = new_m
        refs[18 + i][...] = new_v


def solution(mesh):
    def step(x, dy, *arrays):
        weights, ms, vs = (arrays[i : i + 3] for i in (0, 3, 6))
        hbm = pl.BlockSpec(memory_space=pl.ANY)
        dma = pltpu.SemaphoreType.DMA
        gu, d, sq, _ = pl.pallas_call(
            kernel,
            name="train_step",
            out_shape=(
                jax.ShapeDtypeStruct((L, 2, DS, FF), BF),
                jax.ShapeDtypeStruct((L, FS, D), BF),
                jax.ShapeDtypeStruct((8, 128), F32),
                jax.ShapeDtypeStruct((NC, T, 2 * FC), F32),
            ),
            in_specs=[hbm] * 5,
            out_specs=(hbm, hbm, pl.BlockSpec(memory_space=pltpu.VMEM), hbm),
            scratch_shapes=[
                pltpu.VMEM((T, D), BF),
                pltpu.VMEM((T, D), BF),
                pltpu.VMEM((T, D), BF),
                pltpu.VMEM((T, D), BF),
                pltpu.VMEM((D, T), BF),
                pltpu.VMEM((D, T), BF),
                pltpu.VMEM((T, D), F32),
                pltpu.VMEM((L, 2, D, FF), BF),
                pltpu.VMEM((L, FF, D), BF),
                pltpu.VMEM((3, D, FC), F32),
                pltpu.VMEM((2, 2, D, FC), BF),
                pltpu.VMEM((2, FC, D), BF),
                pltpu.VMEM((2, 2, 2, DS, FC), BF),
                pltpu.VMEM((2, 2, QR, D), BF),
                pltpu.VMEM((G, *GU), BF),
                pltpu.VMEM((G, QR, D), BF),
                pltpu.VMEM((G, *GU), BF),
                pltpu.VMEM((G, QR, D), BF),
                pltpu.VMEM((4, *GU), F32),
                pltpu.VMEM((4, QR, D), F32),
                pltpu.VMEM((G, *GU), BF),
                pltpu.VMEM((G, QR, D), BF),
                pltpu.VMEM((G, 2, DS // 2, FC), BF),
                pltpu.VMEM((G, FC // 8, D), BF),
                pltpu.VMEM((G, 2, 3, 16, FC), BF),
                pltpu.VMEM((G, 3, 16, 256), BF),
                pltpu.VMEM((G, 2, 16, FC), BF),
                pltpu.VMEM((G, 16, 256), BF),
                pltpu.VMEM((L, 2, DS, FF), BF),
                pltpu.VMEM((L, FS, D), BF),
                pltpu.VMEM((8, 128), F32),
                pltpu.VMEM((32, 8, 128), F32),
                pltpu.VMEM((2, 3, TB, 2 * FC), F32),
                dma((2,)), dma((BB,)),
                dma((2,)),
                *[dma((6,))] * 3,
                *[dma((10,))] * 8,
                dma((2, 2)), dma((2, 6)), dma((2,)), dma((G, 3)),
                dma((2,)), dma((G, 3)), dma((2,)), dma((G, 9)),
                dma(()), dma((G, 2)), *[dma(())] * 6, dma((2,)),
            ],
            compiler_params=pltpu.CompilerParams(collective_id=0, has_side_effects=True, vmem_limit_bytes=67043328),
        )(x, dy, *weights)
        wide = pl.BlockSpec((1, DS // STEPS, FF), lambda l, i: (l, i, 0))
        deep = pl.BlockSpec((1, FS // STEPS, D), lambda l, i: (l, i, 0))
        three = [wide, wide, deep]
        gate = pl.BlockSpec((1, 1, DS // STEPS, FF), lambda l, i: (l, 0, i, 0))
        up = pl.BlockSpec((1, 1, DS // STEPS, FF), lambda l, i: (l, 1, i, 0))
        new = pl.pallas_call(
            optimizer,
            name="optimizer",
            grid=(L, STEPS),
            out_shape=[jax.ShapeDtypeStruct(a.shape, t) for t, which in ((BF, weights), (F32, ms), (F32, vs)) for a in which],
            in_specs=[pl.BlockSpec((8, 128), lambda l, i: (0, 0)), gate, up, deep] + three * 3,
            out_specs=three * 3,
            compiler_params=pltpu.CompilerParams(dimension_semantics=("arbitrary", "arbitrary")),
        )(sq, gu, gu, d, *weights, *ms, *vs)
        return tuple(new)

    states, cut = P(("rep", "r", "s")), P(None, "s")
    return jax.shard_map(
        step, mesh=mesh, in_specs=(states, states) + (cut,) * 9, out_specs=(P("rep", "s"),) * 9, check_vma=False
    )
```

```python
import jax
import jax.numpy as jnp
from jax import lax
from jax.experimental import pallas as pl
from jax.experimental.pallas import tpu as pltpu
from jax.sharding import PartitionSpec as P

MESH = pl.DeviceIdType.MESH
BF, F32 = jnp.bfloat16, jnp.float32
ALL, MATRICES, OTHERS, BOTH = slice(None), range(3), range(1, 32), (1, 0)
T, D, FF, L = 4096, 512, 1280, 2
TB, FC = 512, 256
NT, NC = T // TB, FF // FC
TBB, SB = 1024, 256
BB = T // TBB
G = L * NC
STEPS = 1
DS, FS = D // 4, FF // 4
QR, GU = FC // 4, (2, DS, FC)


def dot(a, b):
    return jnp.dot(a, b, preferred_element_type=F32)


def dot_t(a, b):
    return lax.dot_general(a, b, (((1,), (1,)), ((), ())), preferred_element_type=F32)


def sigmoid(g):
    return 0.5 + 0.5 * jnp.tanh(0.5 * g)


def norm_scale(wide):
    return lax.rsqrt(jnp.mean(wide * wide, -1, keepdims=True) + 1e-6)


def aligned(i, n):
    return pl.multiple_of(i * n, n)


def kernel(x_in, dy_in, wg_in, wu_in, wd_in, gu_out, d_out, sq_out, kept, *scratch):
    (hb, dyb, a0, a1, at, dyt, da, wgu, wd, acc, sbg, sbd, r0g, r0d, t1g, t1d, r1g, r1d, o32g, o32d, s2g, s2d, ryg, ryd, r2g, r2d,
     fg, fd, gfin, dfin, sqacc, sq, st, sts, ks, ld, wla, wcs, wcr, wxs, wxr, wys, wyr, was, war, wbs, wbr,
     s0s, s0r, s1s, s1r, sys, syr, s2s, s2r, s3s, s3r, s3ys, s3yr, s3ds, s3dr, sqs, sqr, osem) = scratch
    s, r = lax.axis_index("s"), lax.axis_index("r")
    xx, cc, yy = s // 2, s % 2, r // 4
    s1, s2 = s + 1 - 2 * cc, (s + 2) % 4
    s3 = (s1 + 2) % 4
    across = (r + 4) % 8

    def other(k):
        return {"r": (r + k // 4) % 8, "s": (s + k) % 4}

    def remote(src, dst, send, recv, rr, ss):
        return pltpu.make_async_remote_copy(
            src_ref=src, dst_ref=dst, send_sem=send, recv_sem=recv, device_id={"r": rr, "s": ss}, device_id_type=MESH
        )

    barrier = pltpu.get_barrier_semaphore()
    for k in OTHERS:
        pl.semaphore_signal(barrier, inc=1, device_id=other(k), device_id_type=MESH)

    WIDE = (512, 768)

    def first(part, x):
        return pl.multiple_of((1 - x) * 512, 256) if part else pl.multiple_of(x * 768, 256)

    def shard_in(j):
        return (wg_in, wu_in, wd_in)[j % 3].at[j // 3]

    def region(j, who):
        if j % 3 < 2:
            return wgu.at[j // 3, j % 3, pl.ds(aligned(who, DS), DS), :]
        return wd.at[j // 3, pl.ds(aligned(who, FS), FS), :]

    def own(j):
        return pltpu.make_async_copy(shard_in(j), region(j, s), wla.at[j])

    def to_core(j):
        return remote(region(j, s), region(j, s), wcs.at[j], wcr.at[j], r, s1)

    def half_of(j, who, half, x):
        if j in (2, 7):
            return wd.at[j // 7, pl.ds(aligned(2 * who + half, 160), 160), :]
        rows = pl.ds(aligned(2 * who + half, 64), 64)
        if j < 5:
            return wgu.at[0, j % 3 if j < 2 else j - 3, rows, pl.ds(first(j // 3, x), WIDE[j // 3])]
        return wgu.at[1, (j - 5) % 3, rows, slice(0, FC) if j < 7 else slice(FC, FF)]

    def by_x(j):
        return remote(half_of(j, s, yy, 1 - xx), half_of(j, s, yy, 1 - xx), wxs.at[j], wxr.at[j], r, s2)

    def by_y(j):
        return remote(half_of(j, s2, yy, xx), half_of(j, s2, yy, xx), wys.at[j], wyr.at[j], across, s)

    def by_core(j, half, send, recv):
        return remote(half_of(j, s2, half, xx), half_of(j, s2, half, xx), send.at[j], recv.at[j], r, s1)

    def got_x(j):
        by_x(j).wait_recv()
        by_y(j).start()
        by_core(j, yy, was, war).start()

    def got_y(j):
        by_y(j).wait_recv()
        by_core(j, 1 - yy, wbs, wbr).start()

    def got_core(j):
        by_core(j, yy, was, war).wait_recv()
        by_core(j, 1 - yy, wbs, wbr).wait_recv()

    sqacc[...] = jnp.zeros_like(sqacc)
    for j in range(6):
        own(j).start()
    load_x = pltpu.make_async_copy(x_in.at[0], hb, ld.at[0])
    load_dy = pltpu.make_async_copy(dy_in.at[0], dyb, ld.at[1])
    load_x.start()
    load_dy.start()
    for j in range(6):
        own(j).wait()
    pl.semaphore_wait(barrier, 31)
    for j in range(10):
        by_x(j).start()
    for j in range(6):
        to_core(j).start()
    load_x.wait()
    load_dy.wait()

    def prologue(i, _):
        rows = pl.ds(aligned(i, TB), TB)
        wide = hb[rows, :].astype(F32)
        a = (wide * norm_scale(wide)).astype(BF)
        a0[rows, :] = a
        dyt[:, rows] = dyb[rows, :].T

        @pl.when(i == 5)
        def _():
            got_x(0)

        @pl.when(i == 7)
        def _():
            got_x(1)

        return 0

    lax.fori_loop(0, NT, prologue, 0)

    def mlp(a, start, width, slot):
        o = None
        for c in range(width // FC):
            cols = pl.ds(pl.multiple_of(start + c * FC, FC), FC)
            g = dot(a, wgu[0, 0, :, cols])
            u = dot(a, wgu[0, 1, :, cols])
            st[slot, c, :, :FC] = g
            st[slot, c, :, FC:] = u
            p = (g * sigmoid(g) * u).astype(BF)
            one = dot(p, wd[0, cols, :])
            o = one if o is None else o + one
        return o

    def keep(i, part):
        slot, count = i % 2, WIDE[part] // FC
        return pltpu.make_async_copy(
            st.at[slot, :count],
            kept.at[pl.ds(first(part, xx) // FC, count), pl.ds(aligned(i, TB), TB), :],
            sts.at[slot],
        )

    def free_slot(i, part):
        @pl.when(i >= 2)
        def _():
            keep(i, part).wait()

    def fwd_first(i, _):
        @pl.when(i == 2)
        def _():
            got_x(3)

        @pl.when(i == 5)
        def _():
            got_x(4)

        free_slot(i, 0)
        rows = pl.ds(aligned(i, TB), TB)
        da[rows, :] = mlp(a0[rows, :], first(0, xx), WIDE[0], i % 2)
        keep(i, 0).start()
        return 0

    def fwd_second(i, _):
        @pl.when(i == 0)
        def _():
            for j in (5, 6):
                got_x(j)

        @pl.when(i == 1)
        def _():
            got_x(7)

        @pl.when(i == 2)
        def _():
            got_y(5)
            got_y(6)

        @pl.when(i == 3)
        def _():
            got_x(8)

        @pl.when(i == 5)
        def _():
            got_x(9)
            got_y(7)

        free_slot(i, 1)
        rows = pl.ds(aligned(i, TB), TB)
        o = da[rows, :] + mlp(a0[rows, :], first(1, xx), WIDE[1], i % 2)
        keep(i, 1).start()
        da[rows, :] = jnp.zeros((TB, D), F32)
        h = hb[rows, :] + o.astype(BF)
        hb[rows, :] = h
        wide = h.astype(F32)
        a = (wide * norm_scale(wide)).astype(BF)
        a1[rows, :] = a
        at[:, rows] = a.T
        return 0

    got_y(0)
    got_y(1)
    got_x(2)
    for j in MATRICES:
        to_core(j).wait_recv()
    got_core(0)
    got_core(1)
    lax.fori_loop(0, NT, fwd_first, 0)
    keep(NT - 2, 0).wait()
    keep(NT - 1, 0).wait()
    for get in (got_y, got_core):
        for j in (2, 3, 4):
            get(j)
    lax.fori_loop(0, NT, fwd_second, 0)
    keep(NT - 2, 1).wait()
    keep(NT - 1, 1).wait()
    for j in range(3, 6):
        to_core(j).wait_recv()
    for j in (5, 6, 7):
        got_core(j)

    def part(m, who):
        return pl.ds(aligned(who, 64), 64) if m == 2 else pl.ds(aligned(who, DS), DS)

    def mine(m, gu, d):
        return (lambda g, *at: d.at[(g, *at)]) if m == 2 else (lambda g, *at: gu.at[(g, m, *at)])

    def stage0(g, m, w):
        slot = g % 2
        src = mine(m, sbg, sbd)(slot, part(m, (s1, s3)[w]), ALL)
        return remote(src, mine(m, r0g, r0d)(slot, w), s0s.at[slot, m // 2], s0r.at[slot, 2 * m + w], r, s1)

    def stage0_sent(g):
        slot = g % 2
        pltpu.make_async_copy(r0g.at[slot], r0g.at[slot], s0s.at[slot, 0]).wait()
        pltpu.make_async_copy(r0d.at[slot], r0d.at[slot], s0s.at[slot, 1]).wait()

    def stage1(g, m):
        return remote(mine(m, t1g, t1d)(g), mine(m, r1g, r1d)(g), s1s.at[m // 2], s1r.at[g, m], r, s2)

    def piece(m, who):
        if m == 2:
            return pl.ds(aligned(who // 2, 16), 16), pl.ds(aligned(who % 2, 256), 256)
        return pl.ds(aligned(who, 16), 16), ALL

    def half(m, y):
        return pl.ds(aligned(y, 32), 32) if m == 2 else pl.ds(aligned(y, 64), 64)

    def stage2y(g, m):
        return remote(
            mine(m, s2g, s2d)(g, half(m, 1 - yy), ALL), mine(m, ryg, ryd)(g), sys.at[m // 2], syr.at[g, m], across, s
        )

    def stage2(g, m, k):
        to = 4 * yy + (r % 4 + k) % 4
        return remote(
            mine(m, s2g, s2d)(g, *piece(m, to)), mine(m, r2g, r2d)(g, k - 1), s2s.at[m // 2], s2r.at[g, 3 * m + k - 1], to, s
        )

    def place(g):
        block = 4 * (g % NC) + s
        spot = pl.ds(aligned(4 * (block % 5) + r // 2, 16), 16), pl.ds(aligned(r % 2, 256), 256)
        return 1 - g // NC, g % NC, block // 5, spot

    def stage3(g, m, k):
        layer, c, owner, spot = place(g)
        if m == 2:
            return remote(fd.at[g], dfin.at[(layer, *spot)], s3ds, s3dr, (r + k) % 8, owner)
        to = 4 * yy + (r % 4 + k) % 4
        where = gfin.at[layer, m, pl.ds(aligned(r, 16), 16), pl.ds(aligned(c, FC), FC)]
        return remote(fg.at[g, m], where, s3s, s3r.at[g, m], to, s)

    def stage3y(g, m):
        layer, c, _, _ = place(g)
        block = gfin.at[layer, m, pl.ds(aligned(yy, 64), 64), pl.ds(aligned(c, FC), FC)]
        return remote(block, block, s3ys, s3yr, across, s)

    def add3(g, m):
        if m < 2:
            pltpu.make_async_copy(r2g.at[g, m], r2g.at[g, m], s3r.at[g, m]).wait()
            stage3y(g, m).start()

    def add0(g, m):
        slot = g % 2
        for w in BOTH:
            stage0(g, m, w).wait_recv()
        own_term = mine(m, sbg, sbd)
        arrived = mine(m, r0g, r0d)
        other = own_term(slot, part(m, s2), ALL)[...].astype(F32) + arrived(slot, 1)[...].astype(F32)
        mine(m, t1g, t1d)(g)[...] = other.astype(BF)
        stage1(g, m).start()
        kept = own_term(slot, part(m, s), ALL)[...].astype(F32) + arrived(slot, 0)[...].astype(F32)
        mine(m, o32g, o32d)(g % 4)[...] = kept

    def add1(g, m):
        stage1(g, m).wait_recv()
        total = mine(m, o32g, o32d)(g % 4)[...] + mine(m, r1g, r1d)(g)[...].astype(F32)
        mine(m, o32g, o32d)(g % 4)[...] = total
        mine(m, s2g, s2d)(g)[...] = total.astype(BF)
        stage2y(g, m).start()

    def add2y(g, m):
        stage2y(g, m).wait_recv()
        here = half(m, yy), ALL
        total = mine(m, o32g, o32d)(g % 4, *here)[...] + mine(m, ryg, ryd)(g)[...].astype(F32)
        mine(m, o32g, o32d)(g % 4, *here)[...] = total
        mine(m, s2g, s2d)(g, *here)[...] = total.astype(BF)
        for k in (2, 3, 1):
            stage2(g, m, k).start()

    def add2(g, m):
        for k in range(1, 4):
            stage2(g, m, k).wait_recv()
        total = mine(m, o32g, o32d)(g % 4, *piece(m, r))[...]
        for k in MATRICES:
            total += mine(m, r2g, r2d)(g, k)[...].astype(F32)
        total = total.astype(BF)
        mine(m, fg, fd)(g)[...] = total
        square = total.astype(F32)
        square = square * square
        sqacc[...] += square[:8, :128] + square[:8, 128:] + square[8:, :128] + square[8:, 128:]
        layer, c, owner, spot = place(g)
        if m == 2:

            @pl.when(owner == s)
            def _():
                dfin[(layer, *spot)] = total

            @pl.when(owner != s)
            def _():
                stage3(g, m, 0).start()
        else:
            gfin[layer, m, pl.ds(aligned(r, 16), 16), pl.ds(aligned(c, FC), FC)] = total
        for k in (4, 5, 3, 6, 2, 7, 1) if m == 2 else (2, 3, 1):
            stage3(g, m, k).start()

    def recall(c, at_row, count):
        rows = pl.ds(pl.multiple_of(at_row, TB), count)
        return pltpu.make_async_copy(kept.at[c, rows, :], da.at[rows, :], ks.at[at_row // TBB])

    def backward(layer, with_da):
        def chunk(c, _):
            cols = pl.ds(aligned(c, FC), FC)
            n = (1 - layer) * NC + c

            def block(i, _):
                @pl.when((i == 0) & (n >= 2))
                def _():
                    for m in MATRICES:
                        add1(n - 2, m)

                @pl.when((i == 1) & (n >= 4))
                def _():
                    for m in range(2):
                        add3(n - 4, m)

                @pl.when((i == 1) & (n >= 1))
                def _():
                    for m in MATRICES:
                        add0(n - 1, m)

                @pl.when((i == 2) & (n >= 3))
                def _():
                    for m in MATRICES:
                        add2(n - 3, m)

                @pl.when((i == 3) & (n >= 2))
                def _():
                    for m in MATRICES:
                        add2y(n - 2, m)

                if with_da:

                    @pl.when((i == 1) & (n == 0))
                    def _():
                        got_y(8)

                    @pl.when((i == 2) & (n == 0))
                    def _():
                        got_y(9)

                    @pl.when((i == 3) & (n == 0))
                    def _():
                        got_core(8)
                        got_core(9)

                if not with_da:
                    recall(c, i * TBB, TBB).wait()

                def rows(q):
                    return pl.ds(aligned(i * (TBB // SB) + q, SB), SB)

                def front(q):
                    if with_da:
                        a = a1[rows(q), :]
                        g = dot(a, wgu[layer, 0, :, cols])
                        u = dot(a, wgu[layer, 1, :, cols])
                    else:
                        g, u = da[rows(q), :FC], da[rows(q), FC:]
                    dp = dot_t(dyb[rows(q), :], wd[layer, cols, :]).astype(BF).astype(F32)
                    sig = sigmoid(g)
                    sl = g * sig
                    dsl = sig + sl * (1.0 - sig)
                    return (dp * u * dsl).astype(BF), (dp * sl).astype(BF), (sl * u).astype(BF)

                def back(qs, of):
                    for m, left in enumerate((at, at, dyt)):
                        base = jnp.where(i > 0, acc[m], 0.0) if qs[0] == 0 else acc[m]
                        acc[m] = base + sum(dot(left[:, rows(q)], of[q][m]) for q in qs)
                    if with_da:
                        for q in qs:
                            da[rows(q), :] += dot_t(of[q][0], wgu[layer, 0, :, cols]) + dot_t(of[q][1], wgu[layer, 1, :, cols])

                of = [front(q) for q in range(4)]
                back((0, 1), of)
                back((2, 3), of)
                if not with_da:

                    @pl.when(c < NC - 1)
                    def _():
                        recall(c + 1, i * TBB, TBB).start()

                return 0

            lax.fori_loop(0, BB, block, 0)
            slot = n % 2

            @pl.when(n >= 2)
            def _():
                stage0_sent(n)

            for m in MATRICES:
                mine(m, sbg, sbd)(slot)[...] = (acc[m].T if m == 2 else acc[m]).astype(BF)
                for w in BOTH:
                    stage0(n, m, w).start()
            return 0

        lax.fori_loop(0, NC, chunk, 0)

    backward(1, True)

    def norm_back(i, _):
        rows = pl.ds(aligned(i, TB), TB)
        wide = hb[rows, :].astype(F32)
        scale = norm_scale(wide)
        t = da[rows, :].astype(BF).astype(F32)
        back = scale * t - wide * (scale * scale * scale * jnp.mean(t * wide, -1, keepdims=True))
        dh = dyb[rows, :] + back.astype(BF)
        dyb[rows, :] = dh
        dyt[:, rows] = dh.T
        at[:, rows] = a0[rows, :].T
        recall(0, i * TB, TB).start()
        return 0

    lax.fori_loop(0, NT, norm_back, 0)
    backward(0, False)

    for which, g in ((add1, G - 2), (add2, G - 3), (add0, G - 1), (add2y, G - 2), (add3, G - 4), (add1, G - 1), (add2y, G - 1),
                     (add2, G - 2), (add3, G - 3), (add2, G - 1)):
        for m in MATRICES:
            which(g, m)

    me = 4 * r + s
    sq[me] = sqacc[...]
    for k in OTHERS:
        remote(sq.at[me], sq.at[me], sqs, sqr, *other(k).values()).start()

    def bytes_of(ref, sem):
        pltpu.make_async_copy(ref, ref, sem).wait()

    for g in (G - 2, G - 1):
        for m in range(2):
            add3(g, m)
    bytes_of(gfin.at[:, :, :64], s3yr)
    bytes_of(dfin.at[:, :304], s3dr)
    out_g = pltpu.make_async_copy(gfin, gu_out, osem.at[0])
    out_d = pltpu.make_async_copy(dfin, d_out, osem.at[1])
    out_g.start()
    out_d.start()

    bytes_of(sq.at[:31], sqr)
    total = sq[0]
    for j in range(1, 32):
        total += sq[j]
    sq_out[...] = total
    for j in range(6):
        to_core(j).wait_send()
    for j in range(10):
        by_x(j).wait_send()
        by_y(j).wait_send()
        by_core(j, yy, was, war).wait_send()
        by_core(j, 1 - yy, wbs, wbr).wait_send()
    stage0_sent(G - 2)
    stage0_sent(G - 1)
    bytes_of(t1g, s1s.at[0])
    bytes_of(t1d, s1s.at[1])
    bytes_of(ryg, sys.at[0])
    bytes_of(ryd, sys.at[1])
    bytes_of(r2g, s2s.at[0])
    bytes_of(r2d, s2s.at[1])
    bytes_of(r2g, s3s)
    bytes_of(gfin.at[:, :, :64], s3ys)
    bytes_of(dfin.at[:, :304], s3ds)
    bytes_of(sq.at[:31], sqs)
    out_g.wait()
    out_d.wait()


def optimizer(sq_ref, *refs):
    count = 4 * L * (2 * DS * FF + FS * D)
    factor = jnp.minimum(1.0, 0.5 * lax.rsqrt(jnp.sum(sq_ref[...], keepdims=True) / count + 1e-30))
    for i in MATRICES:
        g, w, m, v = (refs[3 * which + i] for which in range(4))
        g = g[...].reshape(w.shape).astype(F32) * factor.reshape(1, 1, 1)
        new_m = 0.9 * m[...] + 0.1 * g
        new_v = 0.95 * v[...] + 0.05 * g * g
        step = new_m * lax.rsqrt(new_v + 1e-8) + 0.1 * w[...].astype(F32)
        refs[12 + i][...] = (w[...].astype(F32) - 0.02 * step).astype(BF)
        refs[15 + i][...] = new_m
        refs[18 + i][...] = new_v


def solution(mesh):
    def step(x, dy, *arrays):
        weights, ms, vs = (arrays[i : i + 3] for i in (0, 3, 6))
        hbm = pl.BlockSpec(memory_space=pl.ANY)
        dma = pltpu.SemaphoreType.DMA
        gu, d, sq, _ = pl.pallas_call(
            kernel,
            name="train_step",
            out_shape=(
                jax.ShapeDtypeStruct((L, 2, DS, FF), BF),
                jax.ShapeDtypeStruct((L, FS, D), BF),
                jax.ShapeDtypeStruct((8, 128), F32),
                jax.ShapeDtypeStruct((NC, T, 2 * FC), F32),
            ),
            in_specs=[hbm] * 5,
            out_specs=(hbm, hbm, pl.BlockSpec(memory_space=pltpu.VMEM), hbm),
            scratch_shapes=[
                pltpu.VMEM((T, D), BF),
                pltpu.VMEM((T, D), BF),
                pltpu.VMEM((T, D), BF),
                pltpu.VMEM((T, D), BF),
                pltpu.VMEM((D, T), BF),
                pltpu.VMEM((D, T), BF),
                pltpu.VMEM((T, D), F32),
                pltpu.VMEM((L, 2, D, FF), BF),
                pltpu.VMEM((L, FF, D), BF),
                pltpu.VMEM((3, D, FC), F32),
                pltpu.VMEM((2, 2, D, FC), BF),
                pltpu.VMEM((2, FC, D), BF),
                pltpu.VMEM((2, 2, 2, DS, FC), BF),
                pltpu.VMEM((2, 2, QR, D), BF),
                pltpu.VMEM((G, *GU), BF),
                pltpu.VMEM((G, QR, D), BF),
                pltpu.VMEM((G, *GU), BF),
                pltpu.VMEM((G, QR, D), BF),
                pltpu.VMEM((4, *GU), F32),
                pltpu.VMEM((4, QR, D), F32),
                pltpu.VMEM((G, *GU), BF),
                pltpu.VMEM((G, QR, D), BF),
                pltpu.VMEM((G, 2, DS // 2, FC), BF),
                pltpu.VMEM((G, FC // 8, D), BF),
                pltpu.VMEM((G, 2, 3, 16, FC), BF),
                pltpu.VMEM((G, 3, 16, 256), BF),
                pltpu.VMEM((G, 2, 16, FC), BF),
                pltpu.VMEM((G, 16, 256), BF),
                pltpu.VMEM((L, 2, DS, FF), BF),
                pltpu.VMEM((L, FS, D), BF),
                pltpu.VMEM((8, 128), F32),
                pltpu.VMEM((32, 8, 128), F32),
                pltpu.VMEM((2, 3, TB, 2 * FC), F32),
                dma((2,)), dma((BB,)),
                dma((2,)),
                *[dma((6,))] * 3,
                *[dma((10,))] * 8,
                dma((2, 2)), dma((2, 6)), dma((2,)), dma((G, 3)),
                dma((2,)), dma((G, 3)), dma((2,)), dma((G, 9)),
                dma(()), dma((G, 2)), *[dma(())] * 6, dma((2,)),
            ],
            compiler_params=pltpu.CompilerParams(collective_id=0, has_side_effects=True, vmem_limit_bytes=67043328),
        )(x, dy, *weights)
        wide = pl.BlockSpec((1, DS // STEPS, FF), lambda l, i: (l, i, 0))
        deep = pl.BlockSpec((1, FS // STEPS, D), lambda l, i: (l, i, 0))
        three = [wide, wide, deep]
        gate = pl.BlockSpec((1, 1, DS // STEPS, FF), lambda l, i: (l, 0, i, 0))
        up = pl.BlockSpec((1, 1, DS // STEPS, FF), lambda l, i: (l, 1, i, 0))
        new = pl.pallas_call(
            optimizer,
            name="optimizer",
            grid=(L, STEPS),
            out_shape=[jax.ShapeDtypeStruct(a.shape, t) for t, which in ((BF, weights), (F32, ms), (F32, vs)) for a in which],
            in_specs=[pl.BlockSpec((8, 128), lambda l, i: (0, 0)), gate, up, deep] + three * 3,
            out_specs=three * 3,
            compiler_params=pltpu.CompilerParams(dimension_semantics=("arbitrary", "arbitrary")),
        )(sq, gu, gu, d, *weights, *ms, *vs)
        return tuple(new)

    states, cut = P(("rep", "r", "s")), P(None, "s")
    return jax.shard_map(
        step, mesh=mesh, in_specs=(states, states) + (cut,) * 9, out_specs=(P("rep", "s"),) * 9, check_vma=False
    )
```
